256 devices in a mesh: gx: 4 (over x), gy: 8 (over z_hi, y), gz: 8 (over z_lo, core).
Axes of the slice: x: 4, y: 4, z: 8 (z_hi: 2, z_lo: 4; z = z_hi * 4 + z_lo), core: 2. Of those that a mesh axis runs over, the one named last changes fastest.
Arguments:
- velocity: float32 [3, 128, 768, 2048], P(None, 'gx', 'gy', 'gz'), may hold values from -6 to 6
Outputs:
- magnitude: float32 [128, 768, 2048], P('gx', ('gy', 'gz'))
- level_one: float32 [64, 384, 1024], P('gx', 'gy')
- level_two: float32 [32, 192, 512], P('gx', 'gy')
- level_three: float32 [16, 96, 256], P('gx', 'gy')
- level_four: float32 [8, 48, 128], P('gx', 'gy')
- level_five: float32 [4, 24, 64], P('gx', 'gy')
The draws below stay inside these ranges and needn't reach their ends.
All inputs are finite; a program needn't handle non-finite values.
Results may differ from the reference program's by a relative error of at most 0.000075.
Values sent between devices are 32-bit elements; how exact they have to be, the bound alone decides.
No kernel may reach another device: no remote copies, remote signals or barrier semaphores. Data moves between devices by JAX's collectives and lax.ppermute only.
A program may use at most 256 MiB of HBM per device.

```python
import jax
import jax.numpy as jnp
from jax import lax

NX = 128
NY = 768
NZ = 2048


def shard_levels(stream_key, extent, cuts, least, top_value):
    loudness, own = 1.0, jax.random.fold_in(stream_key, 6)
    for axis_at, blocks in cuts:
        steps = jnp.exp(jax.random.uniform(jax.random.fold_in(own, axis_at), (blocks,), jnp.float32, least / len(cuts), top_value / len(cuts)))
        loudness = loudness * jnp.repeat(steps, extent[axis_at] // blocks).reshape([-1 if axis == axis_at else 1 for axis in range(len(extent))])
    return loudness


def normal_values(own_key, extent, scale, limit, split=(), held_as=jnp.bfloat16):
    level = shard_levels(own_key, extent, split, -0.22, 0.18) if split else 1.0
    array = jax.random.normal(own_key, extent, jnp.float32) * scale * level
    return jnp.minimum(jnp.maximum(array, -limit), limit).astype(held_as)


def setup_inputs(seed: int = 0) -> dict:
    streams_of = jax.random.split(jax.random.key(seed), 2)
    velocity = normal_values(streams_of[0], (3, NX, NY, NZ), 1.0, 6.0, ((1, 4), (2, 8), (3, 8)), jnp.float32)
    return {"velocity": velocity}


def central(field, axis):
    return (jnp.roll(field, -1, axis) - jnp.roll(field, 1, axis)) * 0.5

def pooled(field):
    rows, cols, depth = field.shape
    blocks = field.reshape(rows // 2, 2, cols // 2, 2, depth // 2, 2)
    return lax.optimization_barrier(jnp.mean(blocks, axis=(1, 3, 5)))

def reference(velocity):
    speed_u = velocity[0]
    speed_v = velocity[1]
    speed_w = velocity[2]
    curl_first = central(speed_w, 1) - central(speed_v, 2)
    curl_second = central(speed_u, 2) - central(speed_w, 0)
    curl_third = central(speed_v, 0) - central(speed_u, 1)
    magnitude = jnp.sqrt(1.0 + curl_first * curl_first + curl_second * curl_second + curl_third * curl_third)
    level_one = pooled(magnitude)
    level_two = pooled(level_one)
    level_three = pooled(level_two)
    level_four = pooled(level_three)
    level_five = pooled(level_four)
    return (magnitude, level_one, level_two, level_three, level_four, level_five)
```

```python
import functools

import jax
import jax.numpy as jnp
from jax import lax
from jax.experimental import pallas as pl
from jax.experimental.pallas import tpu as pltpu
from jax.sharding import PartitionSpec as P


PLANES = 8
HIGHEST = lax.Precision.HIGHEST
F32 = jnp.float32


def pairing(depth):
    row = lax.broadcasted_iota(jnp.int32, (depth, depth // 2), 0)
    col = lax.broadcasted_iota(jnp.int32, (depth, depth // 2), 1)
    return (lax.div(row, jnp.int32(2)) == col).astype(F32)


def pair_lanes(value):
    rows, depth = value.shape
    width = min(depth, 256)
    matrix = pairing(width)
    parts = [
        jnp.dot(value[:, i : i + width], matrix, precision=HIGHEST, preferred_element_type=F32)
        for i in range(0, depth, width)
    ]
    return parts[0] if len(parts) == 1 else jnp.concatenate(parts, axis=1)


def keep_rows(scratch, at, value):
    for t in range(scratch.shape[0]):
        scratch[t, at : at + value.shape[0], :] = value[:, t * 128 : (t + 1) * 128]


def pair_rows(scratch, pairs):
    parts = [
        scratch[t, pl.ds(0, pairs, stride=2), :] + scratch[t, pl.ds(1, pairs, stride=2), :]
        for t in range(scratch.shape[0])
    ]
    return parts[0] if len(parts) == 1 else jnp.concatenate(parts, axis=1)


def ends_kernel(vel, row_first, row_last, lane_first, lane_last):
    step = pl.program_id(0)
    _, planes, rows, depth = vel.shape
    lane = lax.broadcasted_iota(jnp.int32, (rows, 128), 1)
    first = lane_first[...]
    last = lane_last[...]
    for k in range(2):
        for p in range(planes):
            at = k * 32 + step * planes + p
            first = jnp.where(lane == at, pltpu.roll(vel[k, p, :, :128], at, 1), first)
            last = jnp.where(
                lane == at, pltpu.roll(vel[k, p, :, depth - 128 :], lax.rem(at + 1, 128), 1), last
            )
    lane_first[...] = first
    lane_last[...] = last
    for k, comp in enumerate((0, 2)):
        for p in range(planes):
            row_first[k, p : p + 1, :] = vel[comp, p, 0:1, :]
            row_last[k, p : p + 1, :] = vel[comp, p, rows - 1 : rows, :]


def ends(velocity):
    _, X, Y, Z = velocity.shape
    rows = jax.ShapeDtypeStruct((2, X, Z), F32)
    lanes = jax.ShapeDtypeStruct((Y, 128), F32)
    return pl.pallas_call(
        ends_kernel,
        grid=(X // PLANES,),
        in_specs=[pl.BlockSpec((3, PLANES, Y, Z), lambda i: (0, i, 0, 0))],
        out_specs=[
            pl.BlockSpec((2, PLANES, Z), lambda i: (0, i, 0)),
            pl.BlockSpec((2, PLANES, Z), lambda i: (0, i, 0)),
            pl.BlockSpec((Y, 128), lambda i: (0, 0)),
            pl.BlockSpec((Y, 128), lambda i: (0, 0)),
        ],
        out_shape=[rows, rows, lanes, lanes],
        cost_estimate=pl.CostEstimate(flops=4_000_000, bytes_accessed=9_500_000, transcendentals=0),
        name="ends",
    )(velocity)


def curl_kernel(base, stride, edges, n, *refs):
    vel, v_before, v_after, w_before, w_after, y_before, y_after, z_before, z_after = refs[:9]
    refs = refs[9:]
    if edges:
        x_before, x_after = refs[:2]
        refs = refs[3:]
    mag_out, level_out, summed = refs
    block = base + stride * pl.program_id(0)
    _, planes, rows, depth = vel.shape
    each = rows // n
    tall = 2 * each
    lane = lax.broadcasted_iota(jnp.int32, (tall, depth), 1)
    at_first, at_last = lane == 0, lane == depth - 1
    nblocks = 4

    def edge_plane(k, band, side):
        if side < 0:
            near, far = (v_before, w_before)[k - 1], x_before if edges else None
            test = block == 0
        else:
            near, far = (v_after, w_after)[k - 1], x_after if edges else None
            test = block == nblocks - 1
        plane = near[0, 0, band, :]
        if edges:
            plane = jnp.where(test, far[k - 1, band, :], plane)
        return plane

    for pair in range(planes // 2):
        for q in range(rows // tall):
            lo, hi = q * tall, (q + 1) * tall
            band = slice(lo, hi)
            both = []
            for p in (2 * pair, 2 * pair + 1):

                def first_diff(k):
                    ahead = vel[k, p + 1, band, :] if p + 1 < planes else edge_plane(k, band, 1)
                    behind = vel[k, p - 1, band, :] if p > 0 else edge_plane(k, band, -1)
                    return ahead - behind

                def second_diff(k):
                    slot = 0 if k == 0 else 1
                    if lo == 0:
                        behind = jnp.concatenate(
                            [y_before[slot, p : p + 1, :], vel[k, p, 0 : hi - 1, :]], axis=0
                        )
                    else:
                        behind = vel[k, p, lo - 1 : hi - 1, :]
                    if hi == rows:
                        ahead = jnp.concatenate(
                            [vel[k, p, lo + 1 : hi, :], y_after[slot, p : p + 1, :]], axis=0
                        )
                    else:
                        ahead = vel[k, p, lo + 1 : hi + 1, :]
                    return ahead - behind

                def third_diff(k):
                    field = vel[k, p, band, :]
                    at = k * 32 + block * planes + p
                    fill = jnp.concatenate(
                        [
                            pltpu.roll(z_before[band, :], lax.rem(128 - at, 128), 1),
                            pltpu.roll(z_after[band, :], 127 - at, 1),
                        ],
                        axis=1,
                    )
                    ahead = jnp.where(at_last, fill, pltpu.roll(field, depth - 1, 1))
                    behind = jnp.where(at_first, fill, pltpu.roll(field, 1, 1))
                    return ahead - behind

                one = second_diff(2) - third_diff(1)
                two = third_diff(0) - first_diff(2)
                three = first_diff(1) - second_diff(0)
                both.append(jnp.sqrt(1.0 + 0.25 * (one * one + two * two + three * three)))
            even, odd = both
            at = pair * tall
            for half in range(2):
                cut = slice(half * each, (half + 1) * each)
                mag_out[2 * q + half, at : at + tall, :] = jnp.concatenate(
                    [even[cut, :], odd[cut, :]], axis=0
                )
            keep_rows(summed, pair * rows + lo, even + odd)
    level = pair_lanes(pair_rows(summed, planes // 2 * rows // 2)) * 0.125
    level_out[...] = level.reshape(planes // 2, rows // 2, depth // 2)


def curl(velocity, base, stride, count, rows_halo, lanes_halo, planes_halo=None, level=None, n=8):
    _, X, Y, Z = velocity.shape
    each = Y // n
    edges = planes_halo is not None

    def block(i):
        return base + stride * i

    def single(comp, ahead):
        def index(i):
            at = block(i) * PLANES + (PLANES if ahead else -1)
            return (comp, jnp.minimum(jnp.maximum(at, 0), X - 1), 0, 0)

        return pl.BlockSpec((1, 1, Y, Z), index)

    full2 = pl.BlockSpec((2, Y, Z), lambda i: (0, 0, 0))
    row_spec = pl.BlockSpec((2, PLANES, Z), lambda i: (0, block(i), 0))
    lane_spec = pl.BlockSpec((Y, 128), lambda i: (0, 0))
    in_specs = [
        pl.BlockSpec((3, PLANES, Y, Z), lambda i: (0, block(i), 0, 0)),
        single(1, False),
        single(1, True),
        single(2, False),
        single(2, True),
        row_spec,
        row_spec,
        lane_spec,
        lane_spec,
    ]
    args = [velocity] * 5 + [*rows_halo, *lanes_halo]
    aliases = {}
    if edges:
        in_specs += [full2, full2, pl.BlockSpec(memory_space=pl.ANY)]
        args += [*planes_halo, level]
        aliases = {len(args) - 1: 1}
    return pl.pallas_call(
        functools.partial(curl_kernel, base, stride, edges, n),
        grid=(count,),
        in_specs=in_specs,
        out_specs=[
            pl.BlockSpec((n, PLANES * each, Z), lambda i: (0, i, 0)),
            pl.BlockSpec((PLANES // 2, Y // 2, Z // 2), lambda i: (block(i), 0, 0)),
        ],
        out_shape=[
            jax.ShapeDtypeStruct((n, count * PLANES * each, Z), F32),
            jax.ShapeDtypeStruct((X // 2, Y // 2, Z // 2), F32),
        ],
        scratch_shapes=[pltpu.VMEM((Z // 128, PLANES // 2 * Y, 128), F32)],
        input_output_aliases=aliases,
        cost_estimate=pl.CostEstimate(
            flops=20 * count * PLANES * Y * Z,
            bytes_accessed=20 * count * PLANES * Y * Z,
            transcendentals=count * PLANES * Y * Z,
        ),
        name="curl",
    )(*args)


def lay_kernel(*refs):
    blocks, out = refs[0], refs[-1]
    n, _, depth = blocks.shape
    planes, each, _ = out.shape
    for s in range(n):
        for p in range(planes):
            out[p, :, s * depth : (s + 1) * depth] = blocks[s, p * each : (p + 1) * each, :]


def lay(blocks, base, stride, X, pencil=None):
    n, rows, Z = blocks.shape
    each = 12
    count = rows // (PLANES * each)
    in_specs = [pl.BlockSpec((n, PLANES * each, Z), lambda i: (0, i, 0))]
    args = [blocks]
    aliases = {}
    if pencil is not None:
        in_specs.append(pl.BlockSpec(memory_space=pl.ANY))
        args.append(pencil)
        aliases = {1: 0}
    return pl.pallas_call(
        lay_kernel,
        grid=(count,),
        in_specs=in_specs,
        out_specs=pl.BlockSpec((PLANES, each, n * Z), lambda i: (base + stride * i, 0, 0)),
        out_shape=jax.ShapeDtypeStruct((X, each, n * Z), F32),
        input_output_aliases=aliases,
        cost_estimate=pl.CostEstimate(
            flops=rows * Z * n, bytes_accessed=8 * n * rows * Z, transcendentals=0
        ),
        name="lay",
    )(*args)


def levels_kernel(
    where, own, side, near, near_fwd, far, far_fwd, own_p, side_p, near_p, near_fwd_p, far_p,
    far_fwd_p, one, two, three, four, five, s1, s2, s3, s4,
):
    planes, rows, width = own.shape
    chip, core = where[0], where[1]
    left = chip < 2
    chips = (
        chip,
        chip + 1 - 2 * lax.rem(chip, 2),
        jnp.where(left, 2, 1),
        jnp.where(left, 3, 0),
    )
    outer = jnp.logical_or(chip == 0, chip == 3)
    sets = (
        (core, (own, side, (near, near_fwd), (far, far_fwd))),
        (1 - core, (own_p, side_p, (near_p, near_fwd_p), (far_p, far_fwd_p))),
    )

    for of_core, blocks in sets:
        for source, block in zip(chips, blocks):
            at = pl.ds(pl.multiple_of((2 * source + of_core) * width, width), width)
            if isinstance(block, tuple):

                @pl.when(outer)
                def _():
                    one[:, :, at] = block[1][...]

                @pl.when(jnp.logical_not(outer))
                def _():
                    one[:, :, at] = block[0][...]
            else:
                one[:, :, at] = block[...]

    def up(source, scratch, target):
        half = source.shape[0] // 2
        count, depth = source.shape[1], source.shape[2]
        for i in range(half):
            keep_rows(scratch, i * count, source[2 * i] + source[2 * i + 1])
        result = pair_lanes(pair_rows(scratch, half * count // 2)) * 0.125
        for i in range(half):
            target[i] = result[i * (count // 2) : (i + 1) * (count // 2), :]

    up(one, s1, two)
    up(two, s2, three)
    up(three, s3, four)
    up(four, s4, five)


def levels(where, blocks, n=8):
    planes, rows, width = blocks[0].shape
    depth = width * n
    shapes = [(planes >> k, rows >> k, depth >> k) for k in range(5)]
    vmem = pl.BlockSpec(memory_space=pltpu.VMEM)
    return pl.pallas_call(
        levels_kernel,
        in_specs=[pl.BlockSpec(memory_space=pltpu.SMEM)] + [vmem] * len(blocks),
        out_specs=[vmem] * 5,
        out_shape=[jax.ShapeDtypeStruct(s, F32) for s in shapes],
        scratch_shapes=[pltpu.VMEM((s[2] // 128, s[0] // 2 * s[1], 128), F32) for s in shapes[:4]],
        cost_estimate=pl.CostEstimate(
            flops=4 * planes * rows * depth, bytes_accessed=10 * planes * rows * depth, transcendentals=0
        ),
        name="levels",
    )(where, *blocks)


def chip_pairs(pairs):
    return [(2 * a + core, 2 * b + core) for a, b in pairs for core in (0, 1)]


def core_pairs(chips):
    return [(2 * chip + core, 2 * chip + 1 - core) for chip in chips for core in (0, 1)]


def gather(level):
    def send(value, pairs):
        return lax.ppermute(value, "gz", pairs)

    side = send(level, chip_pairs([(0, 1), (1, 0), (2, 3), (3, 2)]))
    near = send(level, chip_pairs([(1, 2), (2, 1)]))
    far = send(level, chip_pairs([(0, 2), (3, 1)]))
    near_fwd = send(near, chip_pairs([(1, 0), (2, 3)]))
    far_fwd = send(far, chip_pairs([(1, 0), (2, 3)]))
    mine = [level, side, near, near_fwd, far, far_fwd]
    chips = [range(4), range(4), (1, 2), (0, 3), (1, 2), (0, 3)]
    return mine + [send(value, core_pairs(which)) for value, which in zip(mine, chips)]


def ring(axis):
    peers = lax.axis_size(axis)
    up = [(i, (i + 1) % peers) for i in range(peers)]
    return up, [(j, i) for i, j in up]


def exchange(first, last, axis):
    up, down = ring(axis)
    return lax.ppermute(last, axis, up), lax.ppermute(first, axis, down)


def on_device(velocity):
    _, X, Y, Z = velocity.shape
    n = lax.axis_size("gz")
    planes_halo = exchange(velocity[1:, 0], velocity[1:, X - 1], "gx")
    row_first, row_last, lane_first, lane_last = ends(velocity)
    lanes_halo = exchange(lane_first, lane_last, "gz")
    rows_halo = exchange(row_first, row_last, "gy")
    mag_a, level = curl(velocity, 1, 1, 2, rows_halo, lanes_halo)
    mag_b, level = curl(velocity, 0, 3, 2, rows_halo, lanes_halo, planes_halo, level)
    got_a = lax.all_to_all(mag_a, "gz", split_axis=0, concat_axis=0, tiled=True)
    got_b = lax.all_to_all(mag_b, "gz", split_axis=0, concat_axis=0, tiled=True)
    at = lax.axis_index("gz")
    where = jnp.stack([at // 2, at % 2]).astype(jnp.int32)
    upper = levels(where, gather(level))
    pencil = lay(got_a, 1, 1, X)
    pencil = lay(got_b, 0, 3, X, pencil)
    return (pencil, *upper)


def solution(mesh):
    in_specs = (P(None, "gx", "gy", "gz"),)
    out_specs = (
        P("gx", ("gy", "gz"), None),
        P("gx", "gy", None),
        P("gx", "gy", None),
        P("gx", "gy", None),
        P("gx", "gy", None),
        P("gx", "gy", None),
    )
    return jax.shard_map(
        on_device, mesh=mesh, in_specs=in_specs, out_specs=out_specs, check_vma=False
    )
```

```python
import functools

import jax
import jax.numpy as jnp
from jax import lax
from jax.experimental import pallas as pl
from jax.experimental.pallas import tpu as pltpu
from jax.sharding import PartitionSpec as P


PLANES = 8
HIGHEST = lax.Precision.HIGHEST
F32 = jnp.float32


def pairing(depth):
    row = lax.broadcasted_iota(jnp.int32, (depth, depth // 2), 0)
    col = lax.broadcasted_iota(jnp.int32, (depth, depth // 2), 1)
    return (lax.div(row, jnp.int32(2)) == col).astype(F32)


def pair_lanes(value):
    _, depth = value.shape
    width = min(depth, 256)
    matrix = pairing(width)
    parts = [
        jnp.dot(value[:, i : i + width], matrix, precision=HIGHEST, preferred_element_type=F32)
        for i in range(0, depth, width)
    ]
    return parts[0] if len(parts) == 1 else jnp.concatenate(parts, axis=1)


def keep_rows(scratch, at, value):
    for t in range(scratch.shape[0]):
        scratch[t, at : at + value.shape[0], :] = value[:, t * 128 : (t + 1) * 128]


def pair_rows(scratch, pairs):
    parts = [
        scratch[t, pl.ds(0, pairs, stride=2), :] + scratch[t, pl.ds(1, pairs, stride=2), :]
        for t in range(scratch.shape[0])
    ]
    return parts[0] if len(parts) == 1 else jnp.concatenate(parts, axis=1)


def ends_kernel(vel, top, bottom, row_first, row_last, lane_first, lane_last):
    step = pl.program_id(0)
    _, planes, rows, depth = vel.shape
    lane = lax.broadcasted_iota(jnp.int32, (rows, 128), 1)
    first = lane_first[...]
    last = lane_last[...]
    for k in range(2):
        for p in range(planes):
            at = k * 32 + step * planes + p
            first = jnp.where(lane == at, pltpu.roll(vel[k, p, :, :128], at, 1), first)
            last = jnp.where(
                lane == at, pltpu.roll(vel[k, p, :, depth - 128 :], lax.rem(at + 1, 128), 1), last
            )
    lane_first[...] = first
    lane_last[...] = last
    for k, comp in enumerate((0, 2)):
        for p in range(planes):
            row_first[k, p : p + 1, :] = top[comp, p, 0:1, :]
            row_last[k, p : p + 1, :] = bottom[comp, p, 7:8, :]


def ends(velocity):
    _, X, Y, Z = velocity.shape
    rows = jax.ShapeDtypeStruct((2, X, Z), F32)
    lanes = jax.ShapeDtypeStruct((Y, 128), F32)
    return pl.pallas_call(
        ends_kernel,
        grid=(X // PLANES,),
        in_specs=[
            pl.BlockSpec((2, PLANES, Y, Z), lambda i: (0, i, 0, 0)),
            pl.BlockSpec((3, PLANES, 8, Z), lambda i: (0, i, 0, 0)),
            pl.BlockSpec((3, PLANES, 8, Z), lambda i: (0, i, Y // 8 - 1, 0)),
        ],
        out_specs=[
            pl.BlockSpec((2, PLANES, Z), lambda i: (0, i, 0)),
            pl.BlockSpec((2, PLANES, Z), lambda i: (0, i, 0)),
            pl.BlockSpec((Y, 128), lambda i: (0, 0)),
            pl.BlockSpec((Y, 128), lambda i: (0, 0)),
        ],
        out_shape=[rows, rows, lanes, lanes],
        cost_estimate=pl.CostEstimate(flops=4_000_000, bytes_accessed=8_000_000, transcendentals=0),
        name="ends",
    )(velocity, velocity, velocity)


def curl_kernel(shifts, pos, vel, v_before, v_after, w_before, w_after, inner, *refs):
    x_before, x_after, y_before, y_after, z_before, z_after = refs[:6]
    mags = refs[-2 - len(shifts) - 1 : -3]
    level_out, summed, turned = refs[-3:]
    half, me = pos[0], pos[1]
    step = pl.program_id(0)
    _, planes, rows, depth = vel.shape
    each = rows // 4
    tall = 2 * each
    tiles = depth // 128
    lane = lax.broadcasted_iota(jnp.int32, (tall, depth), 1)
    at_first, at_last = lane == 0, lane == depth - 1
    lower = half == 0
    at_start = step == 0
    at_end = step == pl.num_programs(0) - 1

    for pair in range(planes // 2):
        for q in range(rows // tall):
            lo, hi = q * tall, (q + 1) * tall
            band = slice(lo, hi)
            both = []
            for p in (2 * pair, 2 * pair + 1):

                def first_diff(k):
                    if p + 1 < planes:
                        ahead = vel[k, p + 1, band, :]
                    else:
                        near = (v_after, w_after)[k - 1][0, 0, band, :]
                        ahead = jnp.where(at_end, x_after[k - 1, band, :], near)
                    if p > 0:
                        behind = vel[k, p - 1, band, :]
                    else:
                        near = (v_before, w_before)[k - 1][0, 0, band, :]
                        behind = jnp.where(at_start, x_before[k - 1, band, :], near)
                    return ahead - behind

                def second_diff(k):
                    slot = 0 if k == 0 else 1
                    if lo == 0:
                        edge = jnp.where(lower, y_before[slot, p : p + 1, :], inner[k, p, 7:8, :])
                        behind = jnp.concatenate([edge, vel[k, p, 0 : hi - 1, :]], axis=0)
                    else:
                        behind = vel[k, p, lo - 1 : hi - 1, :]
                    if hi == rows:
                        edge = jnp.where(lower, inner[k, p, 0:1, :], y_after[slot, p : p + 1, :])
                        ahead = jnp.concatenate([vel[k, p, lo + 1 : hi, :], edge], axis=0)
                    else:
                        ahead = vel[k, p, lo + 1 : hi + 1, :]
                    return ahead - behind

                def third_diff(k):
                    field = vel[k, p, band, :]
                    at = k * 32 + step * planes + p
                    fill = jnp.concatenate(
                        [
                            pltpu.roll(z_before[band, :], lax.rem(128 - at, 128), 1),
                            pltpu.roll(z_after[band, :], 127 - at, 1),
                        ],
                        axis=1,
                    )
                    ahead = jnp.where(at_last, fill, pltpu.roll(field, depth - 1, 1))
                    behind = jnp.where(at_first, fill, pltpu.roll(field, 1, 1))
                    return ahead - behind

                one = second_diff(2) - third_diff(1)
                two = third_diff(0) - first_diff(2)
                three = first_diff(1) - second_diff(0)
                mag = jnp.sqrt(1.0 + 0.25 * (one * one + two * two + three * three))
                both.append(mag)
                for t in range(tiles):
                    turned[t, pl.ds(lo * planes + p, tall, stride=planes), :] = mag[
                        :, t * 128 : (t + 1) * 128
                    ]
            keep_rows(summed, pair * rows + lo, both[0] + both[1])
    level = pair_lanes(pair_rows(summed, planes // 2 * rows // 2)) * 0.125
    level_out[...] = level.reshape(planes // 2, rows // 2, depth // 2)
    size = each * planes
    for m, out in zip(shifts, mags):
        at = pl.multiple_of(size * jnp.bitwise_xor(jnp.bitwise_and(me, 3), m & 3), size)
        for t in range(tiles):
            out[0, t] = turned[t, pl.ds(at, size), :]


def curl(velocity, shifts, pos, halos, level=None):
    _, X, Y, Z = velocity.shape
    H = Y // 2
    each = H // 4
    planes = PLANES
    tiles = Z // 128
    (x_before, x_after), (y_before, y_after), (z_before, z_after) = halos

    def single(comp, shift):
        def index(i, pos):
            at = jnp.minimum(jnp.maximum(i * planes + shift, 0), X - 1)
            return (comp, at, pos[0], 0)

        return pl.BlockSpec((1, 1, H, Z), index)

    plane_spec = pl.BlockSpec((2, H, Z), lambda i, pos: (0, pos[0], 0))
    row_spec = pl.BlockSpec((2, planes, Z), lambda i, pos: (0, i, 0))
    lane_spec = pl.BlockSpec((H, 128), lambda i, pos: (pos[0], 0))
    in_specs = [
        pl.BlockSpec((3, planes, H, Z), lambda i, pos: (0, i, pos[0], 0)),
        single(1, -1),
        single(1, planes),
        single(2, -1),
        single(2, planes),
        pl.BlockSpec((3, planes, 8, Z), lambda i, pos: (0, i, H // 8 - pos[0], 0)),
        plane_spec,
        plane_spec,
        row_spec,
        row_spec,
        lane_spec,
        lane_spec,
    ]
    args = [velocity] * 6 + [x_before, x_after, y_before, y_after, z_before, z_after]
    aliases = {}
    if level is not None:
        in_specs.append(pl.BlockSpec(memory_space=pl.ANY))
        args.append(level)
        aliases = {len(args): len(shifts)}
    mag_spec = pl.BlockSpec((1, tiles, each * planes, 128), lambda i, pos: (i, 0, 0, 0))
    cells = X * H * Z
    return pl.pallas_call(
        functools.partial(curl_kernel, shifts),
        grid_spec=pltpu.PrefetchScalarGridSpec(
            num_scalar_prefetch=1,
            grid=(X // planes,),
            in_specs=in_specs,
            out_specs=[mag_spec] * len(shifts)
            + [pl.BlockSpec((planes // 2, H // 2, Z // 2), lambda i, pos: (i, pos[0], 0))],
            scratch_shapes=[
                pltpu.VMEM((tiles, planes // 2 * H, 128), F32),
                pltpu.VMEM((tiles, planes * H, 128), F32),
            ],
        ),
        out_shape=[jax.ShapeDtypeStruct((X // planes, tiles, each * planes, 128), F32)] * len(shifts)
        + [jax.ShapeDtypeStruct((X // 2, Y // 2, Z // 2), F32)],
        input_output_aliases=aliases,
        cost_estimate=pl.CostEstimate(
            flops=20 * cells, bytes_accessed=20 * cells, transcendentals=cells
        ),
        name="curl",
    )(pos, *args)


def lay_kernel(shifts, pos, *refs):
    count = len(shifts)
    blocks = refs[:count]
    out, placed, sems = refs[-3:]
    _, each, _, depth = placed.shape
    copies = []
    for k, (m, block) in enumerate(zip(shifts, blocks)):
        for b in range(block.shape[0]):
            for t in range(block.shape[1]):
                for y in range(each):
                    placed[k, y, b * 8 : b * 8 + 8, t * 128 : (t + 1) * 128] = block[
                        b, t, y * 8 : y * 8 + 8, :
                    ]
        at = pl.multiple_of(jnp.bitwise_xor(pos[1], m) * depth, depth)
        copy = pltpu.make_async_copy(placed.at[k], out.at[:, :, pl.ds(at, depth)], sems.at[k])
        copy.start()
        copies.append(copy)
    for copy in copies:
        copy.wait()


def lay(blocks, shifts, pos, pencil=None, n=8):
    deep, tiles, rows, width = blocks[0].shape
    X, each, Z = deep * 8, rows // 8, tiles * width
    count = len(shifts)
    vmem = pl.BlockSpec(memory_space=pltpu.VMEM)
    in_specs = [pl.BlockSpec(memory_space=pltpu.SMEM)] + [vmem] * count
    args = [pos, *blocks]
    aliases = {}
    if pencil is not None:
        in_specs.append(pl.BlockSpec(memory_space=pl.ANY))
        args.append(pencil)
        aliases = {count + 1: 0}
    return pl.pallas_call(
        functools.partial(lay_kernel, shifts),
        in_specs=in_specs,
        out_specs=pl.BlockSpec(memory_space=pl.ANY),
        out_shape=jax.ShapeDtypeStruct((each, X, n * Z), F32),
        scratch_shapes=[pltpu.VMEM((count, each, X, Z), F32), pltpu.SemaphoreType.DMA((count,))],
        input_output_aliases=aliases,
        cost_estimate=pl.CostEstimate(
            flops=count * each * X * Z, bytes_accessed=8 * count * each * X * Z, transcendentals=0
        ),
        name="lay",
    )(*args)


def levels_kernel(shifts, pos, *refs):
    blocks = refs[: len(shifts)]
    one, two, three, four, five, s1, s2, s3, s4 = refs[len(shifts) :]
    width = blocks[0].shape[2]
    for m, block in zip(shifts, blocks):
        at = pl.multiple_of(jnp.bitwise_xor(pos[1], m) * width, width)
        one[:, :, pl.ds(at, width)] = block[...]

    def up(planes, scratch):
        half, count = len(planes) // 2, planes[0].shape[0]
        for i in range(half):
            keep_rows(scratch, i * count, planes[2 * i] + planes[2 * i + 1])
        result = pair_lanes(pair_rows(scratch, half * count // 2)) * 0.125
        return [result[i * (count // 2) : (i + 1) * (count // 2), :] for i in range(half)]

    planes = up([one[i] for i in range(one.shape[0])], s1)
    for i, plane in enumerate(planes):
        two[i] = plane
    for target, scratch in ((three, s2), (four, s3), (five, s4)):
        planes = up(planes, scratch)
        for i, plane in enumerate(planes):
            for j in range(plane.shape[0]):
                target[j, i : i + 1, :] = plane[j : j + 1, :]


def levels(blocks, shifts, pos, n=8):
    planes, rows, width = blocks[0].shape
    depth = width * n
    shapes = [(planes >> k, rows >> k, depth >> k) for k in range(5)]
    outs = shapes[:2] + [(r, p, d) for p, r, d in shapes[2:]]
    vmem = pl.BlockSpec(memory_space=pltpu.VMEM)
    return pl.pallas_call(
        functools.partial(levels_kernel, shifts),
        in_specs=[pl.BlockSpec(memory_space=pltpu.SMEM)] + [vmem] * len(blocks),
        out_specs=[vmem] * 5,
        out_shape=[jax.ShapeDtypeStruct(s, F32) for s in outs],
        scratch_shapes=[pltpu.VMEM((s[2] // 128, s[0] // 2 * s[1], 128), F32) for s in shapes[:4]],
        cost_estimate=pl.CostEstimate(
            flops=4 * planes * rows * depth, bytes_accessed=10 * planes * rows * depth, transcendentals=0
        ),
        name="levels",
    )(pos, *blocks)


def swap(value, m):
    return lax.ppermute(value, "gz", [(i, i ^ m) for i in range(lax.axis_size("gz"))])


def exchange(first, last, axis):
    peers = lax.axis_size(axis)
    up = [(i, (i + 1) % peers) for i in range(peers)]
    down = [(j, i) for i, j in up]
    return lax.ppermute(last, axis, up), lax.ppermute(first, axis, down)


def on_device(velocity):
    _, X, _, _ = velocity.shape
    at = lax.axis_index("gz").astype(jnp.int32)
    own = lax.shift_right_logical(at, jnp.int32(2))
    pos_far = jnp.stack([1 - own, at])
    pos_near = jnp.stack([own, at])
    x_halo = exchange(velocity[1:, 0], velocity[1:, X - 1], "gx")
    row_first, row_last, lane_first, lane_last = ends(velocity)
    z_halo = exchange(lane_first, lane_last, "gz")
    y_halo = exchange(row_first, row_last, "gy")
    halos = (x_halo, y_halo, z_halo)
    *far, level = curl(velocity, (4, 5, 6, 7), pos_far, halos)
    *near, level = curl(velocity, (0, 1, 2, 3), pos_near, halos, level)
    levels_by = {0: level}
    levels_by[4] = swap(level, 4)
    levels_by[2] = swap(level, 2)
    levels_by[6] = swap(levels_by[4], 2)
    for m in (0, 4, 2, 6):
        levels_by[m + 1] = swap(levels_by[m], 1)
    got = {0: near[0]}
    for m in range(1, 8):
        got[m] = swap(near[m] if m < 4 else far[m - 4], m)
    upper = levels([levels_by[m] for m in range(8)], tuple(range(8)), pos_near)
    upper = [*upper[:2]] + [jnp.transpose(level, (1, 0, 2)) for level in upper[2:]]
    early, late = EARLY, LATE
    pencil = lay([got[m] for m in early], early, pos_near)
    pencil = lay([got[m] for m in late], late, pos_near, pencil)
    return (jnp.transpose(pencil, (1, 0, 2)), *upper)


EARLY, LATE = (0, 1, 2, 3, 4, 5), (6, 7)


def solution(mesh):
    in_specs = (P(None, "gx", "gy", "gz"),)
    out_specs = (
        P("gx", ("gy", "gz"), None),
        P("gx", "gy", None),
        P("gx", "gy", None),
        P("gx", "gy", None),
        P("gx", "gy", None),
        P("gx", "gy", None),
    )

    return jax.shard_map(
        on_device, mesh=mesh, in_specs=in_specs, out_specs=out_specs, check_vma=False
    )
```

```python
import functools

import jax
import jax.numpy as jnp
from jax import lax
from jax.experimental import pallas as pl
from jax.experimental.pallas import tpu as pltpu
from jax.sharding import PartitionSpec as P


PLANES = 8
HIGHEST = lax.Precision.HIGHEST
F32 = jnp.float32


def pairing(depth):
    row = lax.broadcasted_iota(jnp.int32, (depth, depth // 2), 0)
    col = lax.broadcasted_iota(jnp.int32, (depth, depth // 2), 1)
    return (lax.div(row, jnp.int32(2)) == col).astype(F32)


def pair_lanes(value):
    _, depth = value.shape
    width = min(depth, 256)
    matrix = pairing(width)
    parts = [
        jnp.dot(value[:, i : i + width], matrix, precision=HIGHEST, preferred_element_type=F32)
        for i in range(0, depth, width)
    ]
    return parts[0] if len(parts) == 1 else jnp.concatenate(parts, axis=1)


def keep_rows(scratch, at, value):
    for t in range(scratch.shape[0]):
        scratch[t, at : at + value.shape[0], :] = value[:, t * 128 : (t + 1) * 128]


def pair_rows(scratch, pairs):
    parts = [
        scratch[t, pl.ds(0, pairs, stride=2), :] + scratch[t, pl.ds(1, pairs, stride=2), :]
        for t in range(scratch.shape[0])
    ]
    return parts[0] if len(parts) == 1 else jnp.concatenate(parts, axis=1)


def edges_kernel(v0, v1, w0, w1, ut, ub, wt, wb, x_first, x_last, y_first, y_last):
    for k, (first, last) in enumerate(((v0, v1), (w0, w1))):
        x_first[k] = first[0, 0]
        x_last[k] = last[0, 0]
    for k, (top, bottom) in enumerate(((ut, ub), (wt, wb))):
        for p in range(top.shape[1]):
            y_first[k, p : p + 1, :] = top[0, p, 0:1, :]
            y_last[k, p : p + 1, :] = bottom[0, p, 7:8, :]


def edges(velocity):
    _, X, Y, Z = velocity.shape

    def plane(comp, at):
        return pl.BlockSpec((1, 1, Y, Z), lambda i: (comp, at, 0, 0))

    def rows(comp, at):
        return pl.BlockSpec((1, X, 8, Z), lambda i: (comp, 0, at, 0))

    planes = jax.ShapeDtypeStruct((2, Y, Z), F32)
    lines = jax.ShapeDtypeStruct((2, X, Z), F32)
    return pl.pallas_call(
        edges_kernel,
        grid=(1,),
        in_specs=[plane(1, 0), plane(1, X - 1), plane(2, 0), plane(2, X - 1)]
        + [rows(0, 0), rows(0, Y // 8 - 1), rows(2, 0), rows(2, Y // 8 - 1)],
        out_specs=[pl.BlockSpec(s.shape, lambda i: (0, 0, 0)) for s in (planes, planes, lines, lines)],
        out_shape=[planes, planes, lines, lines],
        cost_estimate=pl.CostEstimate(flops=1_000_000, bytes_accessed=2_000_000, transcendentals=0),
        name="edges",
    )(*[velocity] * 8)


def lanes_at(k, x):
    last = 2 * (k * 32 + x)
    return last, lax.rem(last + 127, 128)


def ends_kernel(vel, lane_first, lane_last):
    step = pl.program_id(0)
    _, planes, rows, depth = vel.shape
    lane = lax.broadcasted_iota(jnp.int32, (rows, 128), 1)
    first = lane_first[...]
    last = lane_last[...]
    for k in range(2):
        for p in range(planes):
            to_last, to_first = lanes_at(k, step * planes + p)
            first = jnp.where(
                lane == to_first, pltpu.roll(vel[k, p, :, :128], to_first, 1), first
            )
            last = jnp.where(
                lane == to_last, pltpu.roll(vel[k, p, :, depth - 128 :], to_last + 1, 1), last
            )
    lane_first[...] = first
    lane_last[...] = last


def ends(velocity):
    _, X, Y, Z = velocity.shape
    lanes = jax.ShapeDtypeStruct((Y, 128), F32)
    spec = pl.BlockSpec((Y, 128), lambda i: (0, 0))
    return pl.pallas_call(
        ends_kernel,
        grid=(X // PLANES,),
        in_specs=[pl.BlockSpec((2, PLANES, Y, Z), lambda i: (0, i, 0, 0))],
        out_specs=[spec, spec],
        out_shape=[lanes, lanes],
        cost_estimate=pl.CostEstimate(flops=4_000_000, bytes_accessed=7_000_000, transcendentals=0),
        name="ends",
    )(velocity)


def curl_kernel(shifts, each, with_level, pos, vel, v_before, v_after, w_before, w_after, *refs):
    above, below, x_before, x_after, y_before, y_after, z_before, z_after = refs[:8]
    count = len(shifts)
    if with_level:
        level_out, turned, summed = refs[-3:]
        mags = refs[-3 - count : -3]
    else:
        turned = refs[-1]
        mags = refs[-1 - count : -1]
    band_at, me, bands = pos[0], pos[1], pos[2]
    step = pl.program_id(0)
    _, planes, rows, depth = vel.shape
    tall = 2 * each
    tiles = depth // 128
    lane = lax.broadcasted_iota(jnp.int32, (tall, depth), 1)
    at_first, at_last = lane == 0, lane == depth - 1
    even_lane = lax.broadcasted_iota(jnp.int32, (tall, 128), 1) % 2 == 0
    at_top, at_bottom = band_at == 0, band_at == bands - 1
    at_start = step == 0
    at_end = step == pl.num_programs(0) - 1

    for pair in range(planes // 2):
        for q in range(rows // tall):
            lo, hi = q * tall, (q + 1) * tall
            band = slice(lo, hi)
            both = []
            fills = jnp.where(even_lane, z_before[band, :], z_after[band, :])
            for p in (2 * pair, 2 * pair + 1):

                def first_diff(k):
                    if p + 1 < planes:
                        ahead = vel[k, p + 1, band, :]
                    else:
                        near = (v_after, w_after)[k - 1][0, 0, band, :]
                        ahead = jnp.where(at_end, x_after[k - 1, band, :], near)
                    if p > 0:
                        behind = vel[k, p - 1, band, :]
                    else:
                        near = (v_before, w_before)[k - 1][0, 0, band, :]
                        behind = jnp.where(at_start, x_before[k - 1, band, :], near)
                    return ahead - behind

                def second_diff(k):
                    slot = 0 if k == 0 else 1
                    if lo == 0:
                        edge = jnp.where(at_top, y_before[slot, p : p + 1, :], above[k, p, 7:8, :])
                        behind = jnp.concatenate([edge, vel[k, p, 0 : hi - 1, :]], axis=0)
                    else:
                        behind = vel[k, p, lo - 1 : hi - 1, :]
                    if hi == rows:
                        edge = jnp.where(at_bottom, y_after[slot, p : p + 1, :], below[k, p, 0:1, :])
                        ahead = jnp.concatenate([vel[k, p, lo + 1 : hi, :], edge], axis=0)
                    else:
                        ahead = vel[k, p, lo + 1 : hi + 1, :]
                    return ahead - behind

                def third_diff(k):
                    field = vel[k, p, band, :]
                    last, _ = lanes_at(k, step * planes + p)
                    fill = pltpu.roll(fills, lax.rem(128 - last, 128), 1)
                    fill = jnp.concatenate([fill, fill], axis=1)
                    ahead = jnp.where(at_last, fill, pltpu.roll(field, depth - 1, 1))
                    behind = jnp.where(at_first, fill, pltpu.roll(field, 1, 1))
                    return ahead - behind

                one = second_diff(2) - third_diff(1)
                two = third_diff(0) - first_diff(2)
                three = first_diff(1) - second_diff(0)
                mag = jnp.sqrt(1.0 + 0.25 * (one * one + two * two + three * three))
                both.append(mag)
                for t in range(tiles):
                    turned[t, pl.ds(lo * planes + p, tall, stride=planes), :] = mag[
                        :, t * 128 : (t + 1) * 128
                    ]
            if with_level:
                keep_rows(summed, pair * rows + lo, both[0] + both[1])
    if with_level:
        level = pair_lanes(pair_rows(summed, planes // 2 * rows // 2)) * 0.125
        level_out[...] = level.reshape(planes // 2, rows // 2, depth // 2)
    size = each * planes
    mask = rows // each - 1
    for m, out in zip(shifts, mags):
        at = pl.multiple_of(size * jnp.bitwise_and(jnp.bitwise_xor(me, m), mask), size)
        for t in range(tiles):
            for y in range(each):
                out[y, :, t * 128 : (t + 1) * 128] = turned[t, pl.ds(at + y * planes, planes), :]


def curl(velocity, shifts, pos, bands, halos, level=None, with_level=True, n=8):
    _, X, Y, Z = velocity.shape
    H = Y // bands
    each = Y // n
    planes = PLANES
    tiles = Z // 128
    (x_before, x_after), (y_before, y_after), (z_before, z_after) = halos

    def single(comp, shift):
        def index(i, pos):
            at = jnp.minimum(jnp.maximum(i * planes + shift, 0), X - 1)
            return (comp, at, pos[0], 0)

        return pl.BlockSpec((1, 1, H, Z), index)

    def beside(shift):
        def index(i, pos):
            at = pos[0] * (H // 8) + shift
            return (0, i, jnp.minimum(jnp.maximum(at, 0), Y // 8 - 1), 0)

        return pl.BlockSpec((3, planes, 8, Z), index)

    plane_spec = pl.BlockSpec((2, H, Z), lambda i, pos: (0, pos[0], 0))
    row_spec = pl.BlockSpec((2, planes, Z), lambda i, pos: (0, i, 0))
    lane_spec = pl.BlockSpec((H, 128), lambda i, pos: (pos[0], 0))
    in_specs = [
        pl.BlockSpec((3, planes, H, Z), lambda i, pos: (0, i, pos[0], 0)),
        single(1, -1),
        single(1, planes),
        single(2, -1),
        single(2, planes),
        beside(-1),
        beside(H // 8),
        plane_spec,
        plane_spec,
        row_spec,
        row_spec,
        lane_spec,
        lane_spec,
    ]
    args = [velocity] * 7 + [x_before, x_after, y_before, y_after, z_before, z_after]
    aliases = {}
    out_specs = [pl.BlockSpec((each, planes, Z), lambda i, pos: (0, i, 0))] * len(shifts)
    out_shape = [jax.ShapeDtypeStruct((each, X, Z), F32)] * len(shifts)
    scratch = [pltpu.VMEM((tiles, planes * H, 128), F32)]
    if with_level:
        out_specs.append(pl.BlockSpec((planes // 2, H // 2, Z // 2), lambda i, pos: (i, pos[0], 0)))
        out_shape.append(jax.ShapeDtypeStruct((X // 2, Y // 2, Z // 2), F32))
        scratch.append(pltpu.VMEM((tiles, planes // 2 * H, 128), F32))
        if level is not None:
            in_specs.append(pl.BlockSpec(memory_space=pl.ANY))
            args.append(level)
            aliases = {len(args): len(shifts)}
    cells = X * H * Z
    return pl.pallas_call(
        functools.partial(curl_kernel, shifts, each, with_level),
        grid_spec=pltpu.PrefetchScalarGridSpec(
            num_scalar_prefetch=1,
            grid=(X // planes,),
            in_specs=in_specs,
            out_specs=out_specs,
            scratch_shapes=scratch,
        ),
        out_shape=out_shape,
        input_output_aliases=aliases,
        cost_estimate=pl.CostEstimate(
            flops=20 * cells, bytes_accessed=20 * cells, transcendentals=cells
        ),
        name="curl",
    )(pos, *args)


def lay_kernel(shifts, pos, *refs):
    blocks = refs[: len(shifts)]
    out, placed, into, away = refs[-4:]
    depth = blocks[0].shape[2]
    fetches = [
        pltpu.make_async_copy(block, placed.at[k], into.at[k]) for k, block in enumerate(blocks)
    ]
    for fetch in fetches:
        fetch.start()
    copies = []
    for k, m in enumerate(shifts):
        fetches[k].wait()
        at = pl.multiple_of(jnp.bitwise_xor(pos[1], m) * depth, depth)
        copy = pltpu.make_async_copy(placed.at[k], out.at[:, :, pl.ds(at, depth)], away.at[k])
        copy.start()
        copies.append(copy)
    for copy in copies:
        copy.wait()


def lay(blocks, shifts, pos, pencil=None, n=8):
    each, X, Z = blocks[0].shape
    count = len(shifts)
    anywhere = pl.BlockSpec(memory_space=pl.ANY)
    in_specs = [pl.BlockSpec(memory_space=pltpu.SMEM)] + [anywhere] * count
    args = [pos, *blocks]
    aliases = {}
    if pencil is not None:
        in_specs.append(anywhere)
        args.append(pencil)
        aliases = {count + 1: 0}
    return pl.pallas_call(
        functools.partial(lay_kernel, shifts),
        in_specs=in_specs,
        out_specs=anywhere,
        out_shape=jax.ShapeDtypeStruct((each, X, n * Z), F32),
        scratch_shapes=[
            pltpu.VMEM((count, each, X, Z), F32),
            pltpu.SemaphoreType.DMA((count,)),
            pltpu.SemaphoreType.DMA((count,)),
        ],
        input_output_aliases=aliases,
        cost_estimate=pl.CostEstimate(
            flops=count * each * X * Z, bytes_accessed=8 * count * each * X * Z, transcendentals=0
        ),
        name="lay",
    )(*args)


def levels_kernel(pos, *refs):
    blocks = refs[:8]
    one, two, three, four, five, s1, s2, s3, s4 = refs[8:]
    width = blocks[0].shape[2]
    me = pos[1]
    near = jnp.where(me < 4, 4, 2) + jnp.bitwise_and(me, 1)
    far = jnp.where(me < 4, 6, 0) + jnp.bitwise_and(me, 1)
    sources = (me, jnp.bitwise_xor(me, 2), near, far)
    for k, block in enumerate(blocks):
        source = jnp.bitwise_xor(sources[k % 4], k // 4)
        at = pl.multiple_of(source * width, width)
        one[:, :, pl.ds(at, width)] = block[...]

    def up(planes, scratch):
        half, count = len(planes) // 2, planes[0].shape[0]
        for i in range(half):
            keep_rows(scratch, i * count, planes[2 * i] + planes[2 * i + 1])
        result = pair_lanes(pair_rows(scratch, half * count // 2)) * 0.125
        return [result[i * (count // 2) : (i + 1) * (count // 2), :] for i in range(half)]

    planes = up([one[i] for i in range(one.shape[0])], s1)
    for i, plane in enumerate(planes):
        two[i] = plane
    for target, scratch in ((three, s2), (four, s3), (five, s4)):
        planes = up(planes, scratch)
        for i, plane in enumerate(planes):
            for j in range(plane.shape[0]):
                target[j, i : i + 1, :] = plane[j : j + 1, :]


def levels(blocks, pos, n=8):
    planes, rows, width = blocks[0].shape
    depth = width * n
    shapes = [(planes >> k, rows >> k, depth >> k) for k in range(5)]
    outs = shapes[:2] + [(r, p, d) for p, r, d in shapes[2:]]
    vmem = pl.BlockSpec(memory_space=pltpu.VMEM)
    return pl.pallas_call(
        levels_kernel,
        in_specs=[pl.BlockSpec(memory_space=pltpu.SMEM)] + [vmem] * len(blocks),
        out_specs=[vmem] * 5,
        out_shape=[jax.ShapeDtypeStruct(s, F32) for s in outs],
        scratch_shapes=[pltpu.VMEM((s[2] // 128, s[0] // 2 * s[1], 128), F32) for s in shapes[:4]],
        cost_estimate=pl.CostEstimate(
            flops=4 * planes * rows * depth, bytes_accessed=10 * planes * rows * depth, transcendentals=0
        ),
        name="levels",
    )(pos, *blocks)


def send(value, pairs):
    return lax.ppermute(value, "gz", pairs)


def swap(value, m):
    return send(value, [(i, i ^ m) for i in range(lax.axis_size("gz"))])


def chips(value, pairs):
    return send(value, [(2 * a + core, 2 * b + core) for a, b in pairs for core in (0, 1)])


def exchange(first, last, axis):
    peers = lax.axis_size(axis)
    up = [(i, (i + 1) % peers) for i in range(peers)]
    down = [(j, i) for i, j in up]
    return lax.ppermute(last, axis, up), lax.ppermute(first, axis, down)


def on_device(velocity):
    at = lax.axis_index("gz").astype(jnp.int32)
    own = lax.shift_right_logical(at, jnp.int32(2))
    pos_first = jnp.stack([lax.shift_right_logical(at, jnp.int32(1)) ^ 2, at, jnp.int32(4)])
    pos_far = jnp.stack([1 - own, at, jnp.int32(2)])
    pos_near = jnp.stack([own, at, jnp.int32(2)])
    x_first, x_last, y_first, y_last = edges(velocity)
    x_halo = exchange(x_first, x_last, "gx")
    y_halo = exchange(y_first, y_last, "gy")
    lane_first, lane_last = ends(velocity)
    z_halo = exchange(lane_first, lane_last, "gz")
    halos = (x_halo, y_halo, z_halo)
    blocks = {}
    blocks[4], blocks[5] = curl(velocity, (4, 5), pos_first, 4, halos, with_level=False)
    blocks[6], blocks[7], level = curl(velocity, (6, 7), pos_far, 2, halos)
    *near, level = curl(velocity, (0, 1, 2, 3), pos_near, 2, halos, level)
    blocks.update(enumerate(near))
    side = swap(level, 2)
    across = [(1, 2), (2, 1)]
    outward = [(1, 0), (2, 3)]
    close = chips(level, across)
    distant = chips(side, across)
    close_out = chips(close, outward)
    distant_out = chips(distant, outward)
    mine = [level, side, close + close_out, distant + distant_out]
    theirs = [swap(value, 1) for value in mine]
    got = {0: blocks[0]}
    for m in range(1, 8):
        got[m] = swap(blocks[m], m)
    upper = levels([*mine, *theirs], pos_near)
    upper = [*upper[:2]] + [jnp.transpose(value, (1, 0, 2)) for value in upper[2:]]
    pencil = None
    for which in LAYS:
        pencil = lay([got[m] for m in which], which, pos_near, pencil)
    return (jnp.transpose(pencil, (1, 0, 2)), *upper)


LAYS = ((0, 1, 2, 3, 4, 5), (6,), (7,))


def solution(mesh):
    in_specs = (P(None, "gx", "gy", "gz"),)
    out_specs = (
        P("gx", ("gy", "gz"), None),
        P("gx", "gy", None),
        P("gx", "gy", None),
        P("gx", "gy", None),
        P("gx", "gy", None),
        P("gx", "gy", None),
    )

    return jax.shard_map(
        on_device, mesh=mesh, in_specs=in_specs, out_specs=out_specs, check_vma=False
    )
```

```python
import functools

import jax
import jax.numpy as jnp
from jax import lax
from jax.experimental import pallas as pl
from jax.experimental.pallas import tpu as pltpu
from jax.sharding import PartitionSpec as P


PLANES = 8
HIGHEST = lax.Precision.HIGHEST
F32 = jnp.float32


def pairing(depth):
    row = lax.broadcasted_iota(jnp.int32, (depth, depth // 2), 0)
    col = lax.broadcasted_iota(jnp.int32, (depth, depth // 2), 1)
    return (lax.div(row, jnp.int32(2)) == col).astype(F32)


def pair_lanes(value):
    _, depth = value.shape
    width = min(depth, 256)
    matrix = pairing(width)
    parts = [
        jnp.dot(value[:, i : i + width], matrix, precision=HIGHEST, preferred_element_type=F32)
        for i in range(0, depth, width)
    ]
    return parts[0] if len(parts) == 1 else jnp.concatenate(parts, axis=1)


def keep_rows(scratch, at, value):
    for t in range(scratch.shape[0]):
        scratch[t, at : at + value.shape[0], :] = value[:, t * 128 : (t + 1) * 128]


def pair_rows(scratch, pairs):
    parts = [
        scratch[t, pl.ds(0, pairs, stride=2), :] + scratch[t, pl.ds(1, pairs, stride=2), :]
        for t in range(scratch.shape[0])
    ]
    return parts[0] if len(parts) == 1 else jnp.concatenate(parts, axis=1)


def lanes_at(k, x):
    last = 2 * (k * 32 + x)
    return last, lax.rem(last + 127, 128)


def ends_kernel(
    velocity, x_first, x_last, y_first, y_last, z_first, z_last, uv, w_planes, w_rows, sems
):
    _, X, rows, depth = velocity.shape
    chunk = 4
    chunks = X // chunk
    pieces = [
        (velocity.at[0:2, c * chunk : (c + 1) * chunk], uv.at[:, c * chunk : (c + 1) * chunk])
        for c in range(chunks)
    ]
    pieces += [(velocity.at[2, at], w_planes.at[i]) for i, at in enumerate((0, X - 1))]
    pieces += [
        (velocity.at[2, :, at : at + 8, :], w_rows.at[i]) for i, at in enumerate((0, rows - 8))
    ]
    copies = [pltpu.make_async_copy(a, b, sems.at[i]) for i, (a, b) in enumerate(pieces)]
    for copy in copies:
        copy.start()
    lane = lax.broadcasted_iota(jnp.int32, (rows, 128), 1)
    first = jnp.zeros((rows, 128), F32)
    last = jnp.zeros((rows, 128), F32)
    for c in range(chunks):
        copies[c].wait()
        for p in range(c * chunk, (c + 1) * chunk):
            for k in range(2):
                to_last = 2 * (k * 32 + p)
                to_first = (to_last + 127) % 128
                first = jnp.where(
                    lane == to_first, pltpu.roll(uv[k, p, :, :128], to_first, 1), first
                )
                last = jnp.where(
                    lane == to_last,
                    pltpu.roll(uv[k, p, :, depth - 128 :], (to_last + 1) % 128, 1),
                    last,
                )
            y_first[0, p : p + 1, :] = uv[0, p, 0:1, :]
            y_last[0, p : p + 1, :] = uv[0, p, rows - 1 : rows, :]
    z_first[...] = first
    z_last[...] = last
    for copy in copies[chunks:]:
        copy.wait()
    for i, (out, at) in enumerate(((x_first, 0), (x_last, X - 1))):
        out[0] = uv[1, at]
        out[1] = w_planes[i]
    for p in range(X):
        y_first[1, p : p + 1, :] = w_rows[0, p, 0:1, :]
        y_last[1, p : p + 1, :] = w_rows[1, p, 7:8, :]


def ends(velocity):
    _, X, Y, Z = velocity.shape
    outs = [jax.ShapeDtypeStruct(s, F32) for s in ((2, Y, Z), (2, X, Z), (Y, 128)) for _ in range(2)]
    return pl.pallas_call(
        ends_kernel,
        in_specs=[pl.BlockSpec(memory_space=pl.ANY)],
        out_specs=[pl.BlockSpec(memory_space=pltpu.VMEM)] * 6,
        out_shape=outs,
        scratch_shapes=[
            pltpu.VMEM((2, X, Y, Z), F32),
            pltpu.VMEM((2, Y, Z), F32),
            pltpu.VMEM((2, X, 8, Z), F32),
            pltpu.SemaphoreType.DMA((X // 4 + 4,)),
        ],
        cost_estimate=pl.CostEstimate(flops=4_000_000, bytes_accessed=8_000_000, transcendentals=0),
        name="ends",
    )(velocity)


def curl_kernel(shifts, each, with_level, which, bands, pos, vel, v_before, v_after, w_before, w_after, *refs):
    above, below, x_before, x_after, y_before, y_after, z_before, z_after = refs[:8]
    count = len(shifts)
    if with_level:
        level_out, turned, summed = refs[-3:]
        mags = refs[-3 - count : -3]
    else:
        turned = refs[-1]
        mags = refs[-1 - count : -1]
    band_at, me = pos[which], pos[0]
    step = pl.program_id(0)
    _, planes, rows, depth = vel.shape
    tall = 2 * each
    tiles = depth // 128
    lane = lax.broadcasted_iota(jnp.int32, (tall, depth), 1)
    at_first, at_last = lane == 0, lane == depth - 1
    even_lane = lax.broadcasted_iota(jnp.int32, (tall, 128), 1) % 2 == 0
    at_top, at_bottom = band_at == 0, band_at == bands - 1
    at_start = step == 0
    at_end = step == pl.num_programs(0) - 1

    for pair in range(planes // 2):
        for q in range(rows // tall):
            lo, hi = q * tall, (q + 1) * tall
            band = slice(lo, hi)
            both = []
            fills = jnp.where(even_lane, z_before[band, :], z_after[band, :])
            for p in (2 * pair, 2 * pair + 1):

                def first_diff(k):
                    if p + 1 < planes:
                        ahead = vel[k, p + 1, band, :]
                    else:
                        near = (v_after, w_after)[k - 1][0, 0, band, :]
                        ahead = jnp.where(at_end, x_after[k - 1, band, :], near)
                    if p > 0:
                        behind = vel[k, p - 1, band, :]
                    else:
                        near = (v_before, w_before)[k - 1][0, 0, band, :]
                        behind = jnp.where(at_start, x_before[k - 1, band, :], near)
                    return ahead - behind

                def second_diff(k):
                    slot = 0 if k == 0 else 1
                    if lo == 0:
                        edge = jnp.where(at_top, y_before[slot, p : p + 1, :], above[k, p, 7:8, :])
                        behind = jnp.concatenate([edge, vel[k, p, 0 : hi - 1, :]], axis=0)
                    else:
                        behind = vel[k, p, lo - 1 : hi - 1, :]
                    if hi == rows:
                        edge = jnp.where(at_bottom, y_after[slot, p : p + 1, :], below[k, p, 0:1, :])
                        ahead = jnp.concatenate([vel[k, p, lo + 1 : hi, :], edge], axis=0)
                    else:
                        ahead = vel[k, p, lo + 1 : hi + 1, :]
                    return ahead - behind

                def third_diff(k):
                    field = vel[k, p, band, :]
                    last, _ = lanes_at(k, step * planes + p)
                    fill = pltpu.roll(fills, lax.rem(128 - last, 128), 1)
                    fill = jnp.concatenate([fill, fill], axis=1)
                    ahead = jnp.where(at_last, fill, pltpu.roll(field, depth - 1, 1))
                    behind = jnp.where(at_first, fill, pltpu.roll(field, 1, 1))
                    return ahead - behind

                one = second_diff(2) - third_diff(1)
                two = third_diff(0) - first_diff(2)
                three = first_diff(1) - second_diff(0)
                mag = jnp.sqrt(1.0 + 0.25 * (one * one + two * two + three * three))
                both.append(mag)
                for t in range(tiles):
                    turned[t, pl.ds(lo * planes + p, tall, stride=planes), :] = mag[
                        :, t * 128 : (t + 1) * 128
                    ]
            if with_level:
                keep_rows(summed, pair * rows + lo, both[0] + both[1])
    if with_level:
        level = pair_lanes(pair_rows(summed, planes // 2 * rows // 2)) * 0.125
        level_out[...] = level.reshape(planes // 2, rows // 2, depth // 2)
    size = each * planes
    mask = rows // each - 1
    for m, out in zip(shifts, mags):
        at = pl.multiple_of(size * jnp.bitwise_and(jnp.bitwise_xor(me, m), mask), size)
        for t in range(tiles):
            for y in range(each):
                out[y, :, t * 128 : (t + 1) * 128] = turned[t, pl.ds(at + y * planes, planes), :]


def curl(velocity, shifts, pos, which, bands, halos, level=None, with_level=True, n=8):
    _, X, Y, Z = velocity.shape
    H = Y // bands
    each = Y // n
    planes = PLANES
    tiles = Z // 128
    (x_before, x_after), (y_before, y_after), (z_before, z_after) = halos

    def single(comp, shift):
        def index(i, pos):
            at = jnp.minimum(jnp.maximum(i * planes + shift, 0), X - 1)
            return (comp, at, pos[which], 0)

        return pl.BlockSpec((1, 1, H, Z), index)

    def beside(shift):
        def index(i, pos):
            at = pos[which] * (H // 8) + shift
            return (0, i, jnp.minimum(jnp.maximum(at, 0), Y // 8 - 1), 0)

        return pl.BlockSpec((3, planes, 8, Z), index)

    plane_spec = pl.BlockSpec((2, H, Z), lambda i, pos: (0, pos[which], 0))
    row_spec = pl.BlockSpec((2, planes, Z), lambda i, pos: (0, i, 0))
    lane_spec = pl.BlockSpec((H, 128), lambda i, pos: (pos[which], 0))
    in_specs = [
        pl.BlockSpec((3, planes, H, Z), lambda i, pos: (0, i, pos[which], 0)),
        single(1, -1),
        single(1, planes),
        single(2, -1),
        single(2, planes),
        beside(-1),
        beside(H // 8),
        plane_spec,
        plane_spec,
        row_spec,
        row_spec,
        lane_spec,
        lane_spec,
    ]
    args = [velocity] * 7 + [x_before, x_after, y_before, y_after, z_before, z_after]
    aliases = {}
    out_specs = [pl.BlockSpec((each, planes, Z), lambda i, pos: (0, i, 0))] * len(shifts)
    out_shape = [jax.ShapeDtypeStruct((each, X, Z), F32)] * len(shifts)
    scratch = [pltpu.VMEM((tiles, planes * H, 128), F32)]
    if with_level:
        out_specs.append(pl.BlockSpec((planes // 2, H // 2, Z // 2), lambda i, pos: (i, pos[which], 0)))
        out_shape.append(jax.ShapeDtypeStruct((X // 2, Y // 2, Z // 2), F32))
        scratch.append(pltpu.VMEM((tiles, planes // 2 * H, 128), F32))
        if level is not None:
            in_specs.append(pl.BlockSpec(memory_space=pl.ANY))
            args.append(level)
            aliases = {len(args): len(shifts)}
    cells = X * H * Z
    return pl.pallas_call(
        functools.partial(curl_kernel, shifts, each, with_level, which, bands),
        grid_spec=pltpu.PrefetchScalarGridSpec(
            num_scalar_prefetch=1,
            grid=(X // planes,),
            in_specs=in_specs,
            out_specs=out_specs,
            scratch_shapes=scratch,
        ),
        out_shape=out_shape,
        input_output_aliases=aliases,
        cost_estimate=pl.CostEstimate(
            flops=20 * cells, bytes_accessed=20 * cells, transcendentals=cells
        ),
        name="curl",
    )(pos, *args)


def lay_kernel(shifts, pos, *refs):
    blocks = refs[: len(shifts)]
    out, away = refs[-2:]
    depth = blocks[0].shape[2]
    copies = []
    for k, (m, block) in enumerate(zip(shifts, blocks)):
        at = pl.multiple_of(jnp.bitwise_xor(pos[0], m) * depth, depth)
        copies.append(pltpu.make_async_copy(block, out.at[:, :, pl.ds(at, depth)], away.at[k]))
    for copy in copies:
        copy.start()
    for copy in copies:
        copy.wait()


def lay(blocks, shifts, pos, pencil=None, n=8):
    each, X, Z = blocks[0].shape
    count = len(shifts)
    anywhere = pl.BlockSpec(memory_space=pl.ANY)
    in_specs = [pl.BlockSpec(memory_space=pltpu.SMEM)] + [anywhere] * count
    args = [pos, *blocks]
    aliases = {}
    if pencil is not None:
        in_specs.append(anywhere)
        args.append(pencil)
        aliases = {count + 1: 0}
    return pl.pallas_call(
        functools.partial(lay_kernel, shifts),
        in_specs=in_specs,
        out_specs=anywhere,
        out_shape=jax.ShapeDtypeStruct((each, X, n * Z), F32),
        scratch_shapes=[pltpu.SemaphoreType.DMA((count,))],
        compiler_params=pltpu.CompilerParams(vmem_limit_bytes=1 << 20),
        input_output_aliases=aliases,
        cost_estimate=pl.CostEstimate(
            flops=count * each * X * Z, bytes_accessed=8 * count * each * X * Z, transcendentals=0
        ),
        name="lay",
    )(*args)


def levels_kernel(pos, *refs):
    blocks = refs[:8]
    one, two, three, four, five, s1, s2, s3, s4 = refs[8:]
    width = blocks[0].shape[2]
    me = pos[0]
    near = jnp.where(me < 4, 4, 2) + jnp.bitwise_and(me, 1)
    far = jnp.where(me < 4, 6, 0) + jnp.bitwise_and(me, 1)
    sources = (me, jnp.bitwise_xor(me, 2), near, far)
    for k, block in enumerate(blocks):
        source = jnp.bitwise_xor(sources[k % 4], k // 4)
        at = pl.multiple_of(source * width, width)
        one[:, :, pl.ds(at, width)] = block[...]

    def up(planes, scratch):
        half, count = len(planes) // 2, planes[0].shape[0]
        for i in range(half):
            keep_rows(scratch, i * count, planes[2 * i] + planes[2 * i + 1])
        result = pair_lanes(pair_rows(scratch, half * count // 2)) * 0.125
        return [result[i * (count // 2) : (i + 1) * (count // 2), :] for i in range(half)]

    planes = up([one[i] for i in range(one.shape[0])], s1)
    for i, plane in enumerate(planes):
        two[i] = plane
    for target, scratch in ((three, s2), (four, s3), (five, s4)):
        planes = up(planes, scratch)
        for i, plane in enumerate(planes):
            for j in range(plane.shape[0]):
                target[j, i : i + 1, :] = plane[j : j + 1, :]


def levels(blocks, pos, n=8):
    planes, rows, width = blocks[0].shape
    depth = width * n
    shapes = [(planes >> k, rows >> k, depth >> k) for k in range(5)]
    outs = shapes[:2] + [(r, p, d) for p, r, d in shapes[2:]]
    vmem = pl.BlockSpec(memory_space=pltpu.VMEM)
    return pl.pallas_call(
        levels_kernel,
        in_specs=[pl.BlockSpec(memory_space=pltpu.SMEM)] + [vmem] * len(blocks),
        out_specs=[vmem] * 5,
        out_shape=[jax.ShapeDtypeStruct(s, F32) for s in outs],
        scratch_shapes=[pltpu.VMEM((s[2] // 128, s[0] // 2 * s[1], 128), F32) for s in shapes[:4]],
        cost_estimate=pl.CostEstimate(
            flops=4 * planes * rows * depth, bytes_accessed=10 * planes * rows * depth, transcendentals=0
        ),
        compiler_params=pltpu.CompilerParams(vmem_limit_bytes=24 << 20),
        name="levels",
    )(pos, *blocks)


def send(value, pairs):
    return lax.ppermute(value, "gz", pairs)


def swap(value, m):
    return send(value, [(i, i ^ m) for i in range(lax.axis_size("gz"))])


def chips(value, pairs):
    return send(value, [(2 * a + core, 2 * b + core) for a, b in pairs for core in (0, 1)])


def exchange(first, last, axis):
    peers = lax.axis_size(axis)
    up = [(i, (i + 1) % peers) for i in range(peers)]
    down = [(j, i) for i, j in up]
    return lax.ppermute(last, axis, up), lax.ppermute(first, axis, down)


def on_device(velocity):
    at = lax.axis_index("gz").astype(jnp.int32)
    own = lax.shift_right_logical(at, jnp.int32(2))
    pos = jnp.stack([at, lax.shift_right_logical(at, jnp.int32(1)) ^ 2, 1 - own, own])
    x_first, x_last, y_first, y_last, z_first, z_last = ends(velocity)
    y_halo = exchange(y_first, y_last, "gy")
    x_halo = exchange(x_first, x_last, "gx")
    z_halo = exchange(z_first, z_last, "gz")
    halos = (x_halo, y_halo, z_halo)
    blocks = {}
    blocks[4], blocks[5] = curl(velocity, (4, 5), pos, 1, 4, halos, with_level=False)
    blocks[6], blocks[7], level = curl(velocity, (6, 7), pos, 2, 2, halos)
    *near, level = curl(velocity, (0, 1, 2, 3), pos, 3, 2, halos, level)
    blocks.update(enumerate(near))
    side = swap(level, 2)
    across = [(1, 2), (2, 1)]
    outward = [(1, 0), (2, 3)]
    close = chips(level, across)
    distant = chips(side, across)
    close_out = chips(close, outward)
    distant_out = chips(distant, outward)
    mine = [level, side, close + close_out, distant + distant_out]
    theirs = [swap(value, 1) for value in mine]
    got = {0: blocks[0]}
    for m in range(1, 8):
        got[m] = swap(blocks[m], m)
    upper = levels([*mine, *theirs], pos)
    upper = [*upper[:2]] + [jnp.transpose(value, (1, 0, 2)) for value in upper[2:]]
    pencil = None
    for which in LAYS:
        pencil = lay([got[m] for m in which], which, pos, pencil)
    return (jnp.transpose(pencil, (1, 0, 2)), *upper)


LAYS = ((0, 1, 3, 4, 5), (2, 6), (7,))


def solution(mesh):
    in_specs = (P(None, "gx", "gy", "gz"),)
    out_specs = (
        P("gx", ("gy", "gz"), None),
        P("gx", "gy", None),
        P("gx", "gy", None),
        P("gx", "gy", None),
        P("gx", "gy", None),
        P("gx", "gy", None),
    )

    return jax.shard_map(
        on_device, mesh=mesh, in_specs=in_specs, out_specs=out_specs, check_vma=False
    )
```

```python
import functools

import jax
import jax.numpy as jnp
from jax import lax
from jax.experimental import pallas as pl
from jax.experimental.pallas import tpu as pltpu
from jax.sharding import PartitionSpec as P


PLANES = 8
HIGHEST = lax.Precision.HIGHEST
F32 = jnp.float32


def pairing(depth):
    row = lax.broadcasted_iota(jnp.int32, (depth, depth // 2), 0)
    col = lax.broadcasted_iota(jnp.int32, (depth, depth // 2), 1)
    return (lax.div(row, jnp.int32(2)) == col).astype(F32)


def pair_lanes(value):
    _, depth = value.shape
    width = min(depth, 256)
    matrix = pairing(width)
    parts = [
        jnp.dot(value[:, i : i + width], matrix, precision=HIGHEST, preferred_element_type=F32)
        for i in range(0, depth, width)
    ]
    return parts[0] if len(parts) == 1 else jnp.concatenate(parts, axis=1)


def keep_rows(scratch, at, value):
    for t in range(scratch.shape[0]):
        scratch[t, at : at + value.shape[0], :] = value[:, t * 128 : (t + 1) * 128]


def pair_rows(scratch, pairs):
    parts = [
        scratch[t, pl.ds(0, pairs, stride=2), :] + scratch[t, pl.ds(1, pairs, stride=2), :]
        for t in range(scratch.shape[0])
    ]
    return parts[0] if len(parts) == 1 else jnp.concatenate(parts, axis=1)


def lanes_at(k, x):
    last = 2 * (k * 32 + x)
    return last, lax.rem(last + 127, 128)


def edges_kernel(velocity, x_first, x_last, y_first, y_last, tiles, sems):
    _, X, rows, _ = velocity.shape
    pieces = []
    for k, comp in enumerate((0, 2)):
        for i, at in enumerate((0, rows - 8)):
            pieces.append((velocity.at[comp, :, at : at + 8, :], tiles.at[k, i]))
    for k, comp in enumerate((1, 2)):
        for out, at in ((x_first, 0), (x_last, X - 1)):
            pieces.append((velocity.at[comp, at], out.at[k]))
    copies = [pltpu.make_async_copy(a, b, sems.at[i]) for i, (a, b) in enumerate(pieces)]
    for copy in copies:
        copy.start()
    for copy in copies[:4]:
        copy.wait()
    for k in range(2):
        for p in range(X):
            y_first[k, p : p + 1, :] = tiles[k, 0, p, 0:1, :]
            y_last[k, p : p + 1, :] = tiles[k, 1, p, 7:8, :]
    for copy in copies[4:]:
        copy.wait()


def edges(velocity):
    _, X, Y, Z = velocity.shape
    outs = [jax.ShapeDtypeStruct(s, F32) for s in ((2, Y, Z), (2, X, Z)) for _ in range(2)]
    return pl.pallas_call(
        edges_kernel,
        in_specs=[pl.BlockSpec(memory_space=pl.ANY)],
        out_specs=[pl.BlockSpec(memory_space=pltpu.VMEM)] * 4,
        out_shape=outs,
        scratch_shapes=[pltpu.VMEM((2, 2, X, 8, Z), F32), pltpu.SemaphoreType.DMA((8,))],
        cost_estimate=pl.CostEstimate(flops=1_000_000, bytes_accessed=2_000_000, transcendentals=0),
        name="edges",
    )(velocity)


def ends_kernel(velocity, z_first, z_last, uv, sems):
    _, X, rows, depth = velocity.shape
    chunks = sems.shape[0]
    chunk = X // chunks
    copies = [
        pltpu.make_async_copy(
            velocity.at[0:2, c * chunk : (c + 1) * chunk],
            uv.at[:, c * chunk : (c + 1) * chunk],
            sems.at[c],
        )
        for c in range(chunks)
    ]
    for copy in copies:
        copy.start()
    lane = lax.broadcasted_iota(jnp.int32, (rows, 128), 1)
    first = jnp.zeros((rows, 128), F32)
    last = jnp.zeros((rows, 128), F32)
    for c in range(chunks):
        copies[c].wait()
        for p in range(c * chunk, (c + 1) * chunk):
            for k in range(2):
                to_last = 2 * (k * 32 + p)
                to_first = (to_last + 127) % 128
                first = jnp.where(
                    lane == to_first, pltpu.roll(uv[k, p, :, :128], to_first, 1), first
                )
                last = jnp.where(
                    lane == to_last,
                    pltpu.roll(uv[k, p, :, depth - 128 :], (to_last + 1) % 128, 1),
                    last,
                )
    z_first[...] = first
    z_last[...] = last


def ends(velocity):
    _, X, Y, Z = velocity.shape
    return pl.pallas_call(
        ends_kernel,
        in_specs=[pl.BlockSpec(memory_space=pl.ANY)],
        out_specs=[pl.BlockSpec(memory_space=pltpu.VMEM)] * 2,
        out_shape=[jax.ShapeDtypeStruct((Y, 128), F32)] * 2,
        scratch_shapes=[pltpu.VMEM((2, X, Y, Z), F32), pltpu.SemaphoreType.DMA((X // 4,))],
        cost_estimate=pl.CostEstimate(flops=4_000_000, bytes_accessed=7_000_000, transcendentals=0),
        name="ends",
    )(velocity)


def curl_kernel(shifts, each, with_level, which, bands, pos, vel, v_before, v_after, w_before, w_after, *refs):
    above, below, x_before, x_after, y_before, y_after, z_before, z_after = refs[:8]
    count = len(shifts)
    if with_level:
        level_out, turned, summed = refs[-3:]
        mags = refs[-3 - count : -3]
    else:
        turned = refs[-1]
        mags = refs[-1 - count : -1]
    band_at, me = pos[which], pos[0]
    step = pl.program_id(0)
    _, planes, rows, depth = vel.shape
    tall = 2 * each
    tiles = depth // 128
    lane = lax.broadcasted_iota(jnp.int32, (tall, depth), 1)
    at_first, at_last = lane == 0, lane == depth - 1
    even_lane = lax.broadcasted_iota(jnp.int32, (tall, 128), 1) % 2 == 0
    at_top, at_bottom = band_at == 0, band_at == bands - 1
    at_start = step == 0
    at_end = step == pl.num_programs(0) - 1

    for pair in range(planes // 2):
        for q in range(rows // tall):
            lo, hi = q * tall, (q + 1) * tall
            band = slice(lo, hi)
            both = []
            fills = jnp.where(even_lane, z_before[band, :], z_after[band, :])
            for p in (2 * pair, 2 * pair + 1):

                def first_diff(k):
                    if p + 1 < planes:
                        ahead = vel[k, p + 1, band, :]
                    else:
                        near = (v_after, w_after)[k - 1][0, 0, band, :]
                        ahead = jnp.where(at_end, x_after[k - 1, band, :], near)
                    if p > 0:
                        behind = vel[k, p - 1, band, :]
                    else:
                        near = (v_before, w_before)[k - 1][0, 0, band, :]
                        behind = jnp.where(at_start, x_before[k - 1, band, :], near)
                    return ahead - behind

                def second_diff(k):
                    slot = 0 if k == 0 else 1
                    if lo == 0:
                        edge = jnp.where(at_top, y_before[slot, p : p + 1, :], above[k, p, 7:8, :])
                        behind = jnp.concatenate([edge, vel[k, p, 0 : hi - 1, :]], axis=0)
                    else:
                        behind = vel[k, p, lo - 1 : hi - 1, :]
                    if hi == rows:
                        edge = jnp.where(at_bottom, y_after[slot, p : p + 1, :], below[k, p, 0:1, :])
                        ahead = jnp.concatenate([vel[k, p, lo + 1 : hi, :], edge], axis=0)
                    else:
                        ahead = vel[k, p, lo + 1 : hi + 1, :]
                    return ahead - behind

                def third_diff(k):
                    field = vel[k, p, band, :]
                    last, _ = lanes_at(k, step * planes + p)
                    fill = pltpu.roll(fills, lax.rem(128 - last, 128), 1)
                    fill = jnp.concatenate([fill, fill], axis=1)
                    ahead = jnp.where(at_last, fill, pltpu.roll(field, depth - 1, 1))
                    behind = jnp.where(at_first, fill, pltpu.roll(field, 1, 1))
                    return ahead - behind

                one = second_diff(2) - third_diff(1)
                two = third_diff(0) - first_diff(2)
                three = first_diff(1) - second_diff(0)
                mag = jnp.sqrt(1.0 + 0.25 * (one * one + two * two + three * three))
                both.append(mag)
                for t in range(tiles):
                    turned[t, pl.ds(lo * planes + p, tall, stride=planes), :] = mag[
                        :, t * 128 : (t + 1) * 128
                    ]
            if with_level:
                keep_rows(summed, pair * rows + lo, both[0] + both[1])
    if with_level:
        level = pair_lanes(pair_rows(summed, planes // 2 * rows // 2)) * 0.125
        level_out[...] = level.reshape(planes // 2, rows // 2, depth // 2)
    size = each * planes
    mask = rows // each - 1
    for m, out in zip(shifts, mags):
        at = pl.multiple_of(size * jnp.bitwise_and(jnp.bitwise_xor(me, m), mask), size)
        for t in range(tiles):
            for y in range(each):
                out[y, :, t * 128 : (t + 1) * 128] = turned[t, pl.ds(at + y * planes, planes), :]


def curl(velocity, shifts, pos, which, bands, halos, level=None, with_level=True, n=8):
    _, X, Y, Z = velocity.shape
    H = Y // bands
    each = Y // n
    planes = PLANES
    tiles = Z // 128
    (x_before, x_after), (y_before, y_after), (z_before, z_after) = halos

    def single(comp, shift):
        def index(i, pos):
            at = jnp.minimum(jnp.maximum(i * planes + shift, 0), X - 1)
            return (comp, at, pos[which], 0)

        return pl.BlockSpec((1, 1, H, Z), index)

    def beside(shift):
        def index(i, pos):
            at = pos[which] * (H // 8) + shift
            return (0, i, jnp.minimum(jnp.maximum(at, 0), Y // 8 - 1), 0)

        return pl.BlockSpec((3, planes, 8, Z), index)

    plane_spec = pl.BlockSpec((2, H, Z), lambda i, pos: (0, pos[which], 0))
    row_spec = pl.BlockSpec((2, planes, Z), lambda i, pos: (0, i, 0))
    lane_spec = pl.BlockSpec((H, 128), lambda i, pos: (pos[which], 0))
    in_specs = [
        pl.BlockSpec((3, planes, H, Z), lambda i, pos: (0, i, pos[which], 0)),
        single(1, -1),
        single(1, planes),
        single(2, -1),
        single(2, planes),
        beside(-1),
        beside(H // 8),
        plane_spec,
        plane_spec,
        row_spec,
        row_spec,
        lane_spec,
        lane_spec,
    ]
    args = [velocity] * 7 + [x_before, x_after, y_before, y_after, z_before, z_after]
    aliases = {}
    out_specs = [pl.BlockSpec((each, planes, Z), lambda i, pos: (0, i, 0))] * len(shifts)
    out_shape = [jax.ShapeDtypeStruct((each, X, Z), F32)] * len(shifts)
    scratch = [pltpu.VMEM((tiles, planes * H, 128), F32)]
    if with_level:
        out_specs.append(pl.BlockSpec((planes // 2, H // 2, Z // 2), lambda i, pos: (i, pos[which], 0)))
        out_shape.append(jax.ShapeDtypeStruct((X // 2, Y // 2, Z // 2), F32))
        scratch.append(pltpu.VMEM((tiles, planes // 2 * H, 128), F32))
        if level is not None:
            in_specs.append(pl.BlockSpec(memory_space=pl.ANY))
            args.append(level)
            aliases = {len(args): len(shifts)}
    cells = X * H * Z
    return pl.pallas_call(
        functools.partial(curl_kernel, shifts, each, with_level, which, bands),
        grid_spec=pltpu.PrefetchScalarGridSpec(
            num_scalar_prefetch=1,
            grid=(X // planes,),
            in_specs=in_specs,
            out_specs=out_specs,
            scratch_shapes=scratch,
        ),
        out_shape=out_shape,
        input_output_aliases=aliases,
        cost_estimate=pl.CostEstimate(
            flops=20 * cells, bytes_accessed=20 * cells, transcendentals=cells
        ),
        name="curl",
    )(pos, *args)


def lay_kernel(shifts, pos, *refs):
    blocks = refs[: len(shifts)]
    out, away = refs[-2:]
    depth = blocks[0].shape[2]
    copies = []
    for k, (m, block) in enumerate(zip(shifts, blocks)):
        at = pl.multiple_of(jnp.bitwise_xor(pos[0], m) * depth, depth)
        copies.append(pltpu.make_async_copy(block, out.at[:, :, pl.ds(at, depth)], away.at[k]))
    for copy in copies:
        copy.start()
    for copy in copies:
        copy.wait()


def lay(blocks, shifts, pos, pencil=None, n=8):
    each, X, Z = blocks[0].shape
    count = len(shifts)
    anywhere = pl.BlockSpec(memory_space=pl.ANY)
    in_specs = [pl.BlockSpec(memory_space=pltpu.SMEM)] + [anywhere] * count
    args = [pos, *blocks]
    aliases = {}
    if pencil is not None:
        in_specs.append(anywhere)
        args.append(pencil)
        aliases = {count + 1: 0}
    return pl.pallas_call(
        functools.partial(lay_kernel, shifts),
        in_specs=in_specs,
        out_specs=anywhere,
        out_shape=jax.ShapeDtypeStruct((each, X, n * Z), F32),
        scratch_shapes=[pltpu.SemaphoreType.DMA((count,))],
        compiler_params=pltpu.CompilerParams(vmem_limit_bytes=1 << 20),
        input_output_aliases=aliases,
        cost_estimate=pl.CostEstimate(
            flops=count * each * X * Z, bytes_accessed=8 * count * each * X * Z, transcendentals=0
        ),
        name="lay",
    )(*args)


def levels_kernel(pos, *refs):
    blocks = refs[:8]
    one, two, three, four, five, s1, s2, s3, s4 = refs[8:]
    width = blocks[0].shape[2]
    me = pos[0]
    near = jnp.where(me < 4, 4, 2) + jnp.bitwise_and(me, 1)
    far = jnp.where(me < 4, 6, 0) + jnp.bitwise_and(me, 1)
    sources = (me, jnp.bitwise_xor(me, 2), near, far)
    for k, block in enumerate(blocks):
        source = jnp.bitwise_xor(sources[k % 4], k // 4)
        at = pl.multiple_of(source * width, width)
        one[:, :, pl.ds(at, width)] = block[...]

    def up(planes, scratch):
        half, count = len(planes) // 2, planes[0].shape[0]
        for i in range(half):
            keep_rows(scratch, i * count, planes[2 * i] + planes[2 * i + 1])
        result = pair_lanes(pair_rows(scratch, half * count // 2)) * 0.125
        return [result[i * (count // 2) : (i + 1) * (count // 2), :] for i in range(half)]

    planes = up([one[i] for i in range(one.shape[0])], s1)
    for i, plane in enumerate(planes):
        two[i] = plane
    for target, scratch in ((three, s2), (four, s3), (five, s4)):
        planes = up(planes, scratch)
        for i, plane in enumerate(planes):
            for j in range(plane.shape[0]):
                target[j, i : i + 1, :] = plane[j : j + 1, :]


def levels(blocks, pos, n=8):
    planes, rows, width = blocks[0].shape
    depth = width * n
    shapes = [(planes >> k, rows >> k, depth >> k) for k in range(5)]
    outs = shapes[:2] + [(r, p, d) for p, r, d in shapes[2:]]
    vmem = pl.BlockSpec(memory_space=pltpu.VMEM)
    return pl.pallas_call(
        levels_kernel,
        in_specs=[pl.BlockSpec(memory_space=pltpu.SMEM)] + [vmem] * len(blocks),
        out_specs=[vmem] * 5,
        out_shape=[jax.ShapeDtypeStruct(s, F32) for s in outs],
        scratch_shapes=[pltpu.VMEM((s[2] // 128, s[0] // 2 * s[1], 128), F32) for s in shapes[:4]],
        cost_estimate=pl.CostEstimate(
            flops=4 * planes * rows * depth, bytes_accessed=10 * planes * rows * depth, transcendentals=0
        ),
        compiler_params=pltpu.CompilerParams(vmem_limit_bytes=24 << 20),
        name="levels",
    )(pos, *blocks)


def send(value, pairs):
    return lax.ppermute(value, "gz", pairs)


def swap(value, m):
    return send(value, [(i, i ^ m) for i in range(lax.axis_size("gz"))])


def chips(value, pairs):
    return send(value, [(2 * a + core, 2 * b + core) for a, b in pairs for core in (0, 1)])


def exchange(first, last, axis):
    peers = lax.axis_size(axis)
    up = [(i, (i + 1) % peers) for i in range(peers)]
    down = [(j, i) for i, j in up]
    return lax.ppermute(last, axis, up), lax.ppermute(first, axis, down)


def on_device(velocity):
    at = lax.axis_index("gz").astype(jnp.int32)
    own = lax.shift_right_logical(at, jnp.int32(2))
    pos = jnp.stack([at, lax.shift_right_logical(at, jnp.int32(1)) ^ 2, 1 - own, own])
    x_first, x_last, y_first, y_last = edges(velocity)
    y_halo = exchange(y_first, y_last, "gy")
    x_halo = exchange(x_first, x_last, "gx")
    z_first, z_last = ends(velocity)
    z_halo = exchange(z_first, z_last, "gz")
    halos = (x_halo, y_halo, z_halo)
    blocks = {}
    blocks[4], blocks[5] = curl(velocity, (4, 5), pos, 1, 4, halos, with_level=False)
    blocks[6], blocks[7], level = curl(velocity, (6, 7), pos, 2, 2, halos)
    *near, level = curl(velocity, (0, 1, 2, 3), pos, 3, 2, halos, level)
    blocks.update(enumerate(near))
    side = swap(level, 2)
    across = [(1, 2), (2, 1)]
    outward = [(1, 0), (2, 3)]
    close = chips(level, across)
    distant = chips(side, across)
    close_out = chips(close, outward)
    distant_out = chips(distant, outward)
    mine = [level, side, close + close_out, distant + distant_out]
    theirs = [swap(value, 1) for value in mine]
    got = {0: blocks[0]}
    for m in range(1, 8):
        got[m] = swap(blocks[m], m)
    upper = levels([*mine, *theirs], pos)
    upper = [*upper[:2]] + [jnp.transpose(value, (1, 0, 2)) for value in upper[2:]]
    pencil = None
    for which in LAYS:
        pencil = lay([got[m] for m in which], which, pos, pencil)
    return (jnp.transpose(pencil, (1, 0, 2)), *upper)


LAYS = ((0, 1, 3, 4, 5), (2, 6), (7,))


def solution(mesh):
    in_specs = (P(None, "gx", "gy", "gz"),)
    out_specs = (
        P("gx", ("gy", "gz"), None),
        P("gx", "gy", None),
        P("gx", "gy", None),
        P("gx", "gy", None),
        P("gx", "gy", None),
        P("gx", "gy", None),
    )

    return jax.shard_map(
        on_device, mesh=mesh, in_specs=in_specs, out_specs=out_specs, check_vma=False
    )
```

```python
import functools

import jax
import jax.numpy as jnp
from jax import lax
from jax.experimental import pallas as pl
from jax.experimental.pallas import tpu as pltpu
from jax.sharding import PartitionSpec as P


PLANES = 8
HIGHEST = lax.Precision.HIGHEST
F32 = jnp.float32


def pairing(depth):
    row = lax.broadcasted_iota(jnp.int32, (depth, depth // 2), 0)
    col = lax.broadcasted_iota(jnp.int32, (depth, depth // 2), 1)
    return (lax.div(row, jnp.int32(2)) == col).astype(F32)


def pair_lanes(value):
    _, depth = value.shape
    width = min(depth, 256)
    matrix = pairing(width)
    parts = [
        jnp.dot(value[:, i : i + width], matrix, precision=HIGHEST, preferred_element_type=F32)
        for i in range(0, depth, width)
    ]
    return parts[0] if len(parts) == 1 else jnp.concatenate(parts, axis=1)


def keep_rows(scratch, at, value):
    for t in range(scratch.shape[0]):
        scratch[t, at : at + value.shape[0], :] = value[:, t * 128 : (t + 1) * 128]


def pair_rows(scratch, pairs):
    parts = [
        scratch[t, pl.ds(0, pairs, stride=2), :] + scratch[t, pl.ds(1, pairs, stride=2), :]
        for t in range(scratch.shape[0])
    ]
    return parts[0] if len(parts) == 1 else jnp.concatenate(parts, axis=1)


def lanes_at(k, x):
    last = 2 * (k * 32 + x)
    return last, lax.rem(last + 127, 128)


def ends_kernel(
    velocity, x_first, x_last, y_first, y_last, z_first, z_last, uv, w_planes, w_rows, sems
):
    _, X, rows, depth = velocity.shape
    chunk = 4
    chunks = X // chunk
    pieces = [
        (velocity.at[0:2, c * chunk : (c + 1) * chunk], uv.at[:, c * chunk : (c + 1) * chunk])
        for c in range(chunks)
    ]
    pieces += [(velocity.at[2, at], w_planes.at[i]) for i, at in enumerate((0, X - 1))]
    pieces += [
        (velocity.at[2, :, at : at + 8, :], w_rows.at[i]) for i, at in enumerate((0, rows - 8))
    ]
    copies = [pltpu.make_async_copy(a, b, sems.at[i]) for i, (a, b) in enumerate(pieces)]
    for copy in copies:
        copy.start()
    lane = lax.broadcasted_iota(jnp.int32, (rows, 128), 1)
    first = jnp.zeros((rows, 128), F32)
    last = jnp.zeros((rows, 128), F32)
    for c in range(chunks):
        copies[c].wait()
        for p in range(c * chunk, (c + 1) * chunk):
            for k in range(2):
                to_last = 2 * (k * 32 + p)
                to_first = (to_last + 127) % 128
                first = jnp.where(
                    lane == to_first, pltpu.roll(uv[k, p, :, :128], to_first, 1), first
                )
                last = jnp.where(
                    lane == to_last,
                    pltpu.roll(uv[k, p, :, depth - 128 :], (to_last + 1) % 128, 1),
                    last,
                )
            y_first[0, p : p + 1, :] = uv[0, p, 0:1, :]
            y_last[0, p : p + 1, :] = uv[0, p, rows - 1 : rows, :]
    z_first[...] = first
    z_last[...] = last
    for copy in copies[chunks:]:
        copy.wait()
    for i, (out, at) in enumerate(((x_first, 0), (x_last, X - 1))):
        out[0] = uv[1, at]
        out[1] = w_planes[i]
    for p in range(X):
        y_first[1, p : p + 1, :] = w_rows[0, p, 0:1, :]
        y_last[1, p : p + 1, :] = w_rows[1, p, 7:8, :]


def ends(velocity):
    _, X, Y, Z = velocity.shape
    outs = [jax.ShapeDtypeStruct(s, F32) for s in ((2, Y, Z), (2, X, Z), (Y, 128)) for _ in range(2)]
    return pl.pallas_call(
        ends_kernel,
        in_specs=[pl.BlockSpec(memory_space=pl.ANY)],
        out_specs=[pl.BlockSpec(memory_space=pltpu.VMEM)] * 6,
        out_shape=outs,
        scratch_shapes=[
            pltpu.VMEM((2, X, Y, Z), F32),
            pltpu.VMEM((2, Y, Z), F32),
            pltpu.VMEM((2, X, 8, Z), F32),
            pltpu.SemaphoreType.DMA((X // 4 + 4,)),
        ],
        compiler_params=pltpu.CompilerParams(vmem_limit_bytes=53 << 20),
        cost_estimate=pl.CostEstimate(flops=4_000_000, bytes_accessed=8_000_000, transcendentals=0),
        name="ends",
    )(velocity)


def curl_kernel(shifts, each, with_level, which, bands, pos, vel, v_before, v_after, w_before, w_after, *refs):
    if bands > 1:
        above, below = refs[:2]
        refs = refs[2:]
    x_before, x_after, y_before, y_after, z_before, z_after = refs[:6]
    count = len(shifts)
    if with_level:
        level_out, turned, summed = refs[-3:]
        mags = refs[-3 - count : -3]
    else:
        turned = refs[-1]
        mags = refs[-1 - count : -1]
    band_at, me = pos[which], pos[0]
    step = pl.program_id(0)
    _, planes, rows, depth = vel.shape
    tall = 2 * each
    tiles = depth // 128
    lane = lax.broadcasted_iota(jnp.int32, (tall, 128), 1)
    at_first, at_last, even_lane = lane == 0, lane == 127, lane % 2 == 0
    at_top, at_bottom = band_at == 0, band_at == bands - 1
    at_start = step == 0
    row0 = pl.multiple_of(band_at * rows, 8)
    at_end = step == pl.num_programs(0) - 1

    for pair in range(planes // 2):
        for q in range(rows // tall):
            lo, hi = q * tall, (q + 1) * tall
            band = slice(lo, hi)
            both = []
            here = pl.ds(row0 + lo, tall)
            fills = jnp.where(even_lane, z_before[here, :], z_after[here, :])
            for p in (2 * pair, 2 * pair + 1):

                def first_diff(k):
                    if p + 1 < planes:
                        ahead = vel[k, p + 1, band, :]
                    else:
                        near = (v_after, w_after)[k - 1][0, 0, band, :]
                        ahead = jnp.where(at_end, x_after[k - 1, here, :], near)
                    if p > 0:
                        behind = vel[k, p - 1, band, :]
                    else:
                        near = (v_before, w_before)[k - 1][0, 0, band, :]
                        behind = jnp.where(at_start, x_before[k - 1, here, :], near)
                    return ahead - behind

                def second_diff(k):
                    slot = 0 if k == 0 else 1
                    if lo == 0:
                        edge = y_before[slot, pl.ds(step * planes + p, 1), :]
                        if bands > 1:
                            edge = jnp.where(at_top, edge, above[k, p, 7:8, :])
                        behind = jnp.concatenate([edge, vel[k, p, 0 : hi - 1, :]], axis=0)
                    else:
                        behind = vel[k, p, lo - 1 : hi - 1, :]
                    if hi == rows:
                        edge = y_after[slot, pl.ds(step * planes + p, 1), :]
                        if bands > 1:
                            edge = jnp.where(at_bottom, edge, below[k, p, 0:1, :])
                        ahead = jnp.concatenate([vel[k, p, lo + 1 : hi, :], edge], axis=0)
                    else:
                        ahead = vel[k, p, lo + 1 : hi + 1, :]
                    return ahead - behind

                def third_diff(k):
                    last, _ = lanes_at(k, step * planes + p)
                    fill = pltpu.roll(fills, lax.rem(128 - last, 128), 1)
                    parts = [vel[k, p, band, t * 128 : (t + 1) * 128] for t in range(tiles)]
                    on = [pltpu.roll(part, 127, 1) for part in parts] + [fill]
                    back = [fill] + [pltpu.roll(part, 1, 1) for part in parts]
                    return jnp.concatenate(
                        [
                            jnp.where(at_last, on[t + 1], on[t])
                            - jnp.where(at_first, back[t], back[t + 1])
                            for t in range(tiles)
                        ],
                        axis=1,
                    )

                one = second_diff(2) - third_diff(1)
                two = third_diff(0) - first_diff(2)
                three = first_diff(1) - second_diff(0)
                square = 1.0 + 0.25 * (one * one + two * two + three * three)
                mag = square * lax.rsqrt(square)
                both.append(mag)
                for t in range(tiles):
                    turned[t, pl.ds(lo * planes + p, tall, stride=planes), :] = mag[
                        :, t * 128 : (t + 1) * 128
                    ]
            if with_level:
                keep_rows(summed, pair * rows + lo, both[0] + both[1])
    if with_level:
        level = pair_lanes(pair_rows(summed, planes // 2 * rows // 2)) * 0.125
        level_out[...] = level.reshape(planes // 2, rows // 2, depth // 2)
    size = each * planes
    mask = rows // each - 1
    for m, out in zip(shifts, mags):
        at = pl.multiple_of(size * jnp.bitwise_and(jnp.bitwise_xor(me, m), mask), size)
        for t in range(tiles):
            for y in range(each):
                out[y, :, t * 128 : (t + 1) * 128] = turned[t, pl.ds(at + y * planes, planes), :]


def curl(velocity, shifts, pos, which, bands, halos, with_level=True, n=8):
    _, X, Y, Z = velocity.shape
    H = Y // bands
    each = Y // n
    planes = PLANES
    tiles = Z // 128
    (x_before, x_after), (y_before, y_after), (z_before, z_after) = halos

    def single(comp, shift):
        def index(i, pos):
            at = jnp.minimum(jnp.maximum(i * planes + shift, 0), X - 1)
            return (comp, at, pos[which], 0)

        return pl.BlockSpec((1, 1, H, Z), index)

    def beside(shift):
        def index(i, pos):
            at = pos[which] * (H // 8) + shift
            return (0, i, jnp.minimum(jnp.maximum(at, 0), Y // 8 - 1), 0)

        return pl.BlockSpec((3, planes, 8, Z), index)

    in_specs = [
        pl.BlockSpec((3, planes, H, Z), lambda i, pos: (0, i, pos[which], 0)),
        single(1, -1),
        single(1, planes),
        single(2, -1),
        single(2, planes),
        *([beside(-1), beside(H // 8)] if bands > 1 else []),
        *[pl.BlockSpec(memory_space=pltpu.VMEM)] * 6,
    ]
    args = [velocity] * (7 if bands > 1 else 5) + [x_before, x_after, y_before, y_after, z_before, z_after]
    out_specs = [pl.BlockSpec((each, planes, Z), lambda i, pos: (0, i, 0))] * len(shifts)
    out_shape = [jax.ShapeDtypeStruct((each, X, Z), F32)] * len(shifts)
    scratch = [pltpu.VMEM((tiles, planes * H, 128), F32)]
    if with_level:
        out_specs.append(pl.BlockSpec((planes // 2, H // 2, Z // 2), lambda i, pos: (i, pos[which], 0)))
        out_shape.append(jax.ShapeDtypeStruct((X // 2, Y // 2, Z // 2), F32))
        scratch.append(pltpu.VMEM((tiles, planes // 2 * H, 128), F32))
    cells = X * H * Z
    return pl.pallas_call(
        functools.partial(curl_kernel, shifts, each, with_level, which, bands),
        grid_spec=pltpu.PrefetchScalarGridSpec(
            num_scalar_prefetch=1,
            grid=(X // planes,),
            in_specs=in_specs,
            out_specs=out_specs,
            scratch_shapes=scratch,
        ),
        out_shape=out_shape,
        compiler_params=pltpu.CompilerParams(vmem_limit_bytes=50 << 20),
        cost_estimate=pl.CostEstimate(
            flops=20 * cells, bytes_accessed=20 * cells, transcendentals=cells
        ),
        name="curl",
    )(pos, *args)


def lay_kernel(shifts, pos, *refs):
    blocks = refs[: len(shifts)]
    out, away = refs[-2:]
    depth = blocks[0].shape[2]
    copies = []
    for k, (m, block) in enumerate(zip(shifts, blocks)):
        at = pl.multiple_of(jnp.bitwise_xor(pos[0], m) * depth, depth)
        copies.append(pltpu.make_async_copy(block, out.at[:, :, pl.ds(at, depth)], away.at[k]))
    for copy in copies:
        copy.start()
    for copy in copies:
        copy.wait()


def lay(blocks, shifts, pos, pencil=None, n=8):
    each, X, Z = blocks[0].shape
    count = len(shifts)
    anywhere = pl.BlockSpec(memory_space=pl.ANY)
    in_specs = [pl.BlockSpec(memory_space=pltpu.SMEM)] + [anywhere] * count
    args = [pos, *blocks]
    aliases = {}
    if pencil is not None:
        in_specs.append(anywhere)
        args.append(pencil)
        aliases = {count + 1: 0}
    return pl.pallas_call(
        functools.partial(lay_kernel, shifts),
        in_specs=in_specs,
        out_specs=anywhere,
        out_shape=jax.ShapeDtypeStruct((each, X, n * Z), F32),
        scratch_shapes=[pltpu.SemaphoreType.DMA((count,))],
        compiler_params=pltpu.CompilerParams(vmem_limit_bytes=1 << 20),
        input_output_aliases=aliases,
        cost_estimate=pl.CostEstimate(
            flops=count * each * X * Z, bytes_accessed=8 * count * each * X * Z, transcendentals=0
        ),
        name="lay",
    )(*args)


def levels_kernel(pos, *refs):
    blocks = refs[:8]
    one, two, three, four, five, s1, s2, s3, s4 = refs[8:]
    width = blocks[0].shape[2]
    me = pos[0]
    near = jnp.where(me < 4, 4, 2) + jnp.bitwise_and(me, 1)
    far = jnp.where(me < 4, 6, 0) + jnp.bitwise_and(me, 1)
    sources = (me, jnp.bitwise_xor(me, 2), near, far)
    for k, block in enumerate(blocks):
        source = jnp.bitwise_xor(sources[k % 4], k // 4)
        at = pl.multiple_of(source * width, width)
        one[:, :, pl.ds(at, width)] = block[...]

    def up(planes, scratch):
        half, count = len(planes) // 2, planes[0].shape[0]
        for i in range(half):
            keep_rows(scratch, i * count, planes[2 * i] + planes[2 * i + 1])
        result = pair_lanes(pair_rows(scratch, half * count // 2)) * 0.125
        return [result[i * (count // 2) : (i + 1) * (count // 2), :] for i in range(half)]

    planes = up([one[i] for i in range(one.shape[0])], s1)
    for i, plane in enumerate(planes):
        two[i] = plane
    for target, scratch in ((three, s2), (four, s3), (five, s4)):
        planes = up(planes, scratch)
        for i, plane in enumerate(planes):
            for j in range(plane.shape[0]):
                target[j, i : i + 1, :] = plane[j : j + 1, :]


def levels(blocks, pos, n=8):
    planes, rows, width = blocks[0].shape
    depth = width * n
    shapes = [(planes >> k, rows >> k, depth >> k) for k in range(5)]
    outs = shapes[:2] + [(r, p, d) for p, r, d in shapes[2:]]
    vmem = pl.BlockSpec(memory_space=pltpu.VMEM)
    return pl.pallas_call(
        levels_kernel,
        in_specs=[pl.BlockSpec(memory_space=pltpu.SMEM)] + [vmem] * len(blocks),
        out_specs=[vmem] * 5,
        out_shape=[jax.ShapeDtypeStruct(s, F32) for s in outs],
        scratch_shapes=[pltpu.VMEM((s[2] // 128, s[0] // 2 * s[1], 128), F32) for s in shapes[:4]],
        cost_estimate=pl.CostEstimate(
            flops=4 * planes * rows * depth, bytes_accessed=10 * planes * rows * depth, transcendentals=0
        ),
        compiler_params=pltpu.CompilerParams(vmem_limit_bytes=24 << 20),
        name="levels",
    )(pos, *blocks)


def send(value, pairs):
    return lax.ppermute(value, "gz", pairs)


def swap(value, m):
    return send(value, [(i, i ^ m) for i in range(lax.axis_size("gz"))])


def chips(value, pairs):
    return send(value, [(2 * a + core, 2 * b + core) for a, b in pairs for core in (0, 1)])


def exchange(first, last, axis):
    peers = lax.axis_size(axis)
    up = [(i, (i + 1) % peers) for i in range(peers)]
    down = [(j, i) for i, j in up]
    return lax.ppermute(last, axis, up), lax.ppermute(first, axis, down)


def on_device(velocity):
    at = lax.axis_index("gz").astype(jnp.int32)
    pos = jnp.stack([at, lax.shift_right_logical(at, jnp.int32(1)) ^ 2, jnp.int32(0)])
    x_first, x_last, y_first, y_last, z_first, z_last = ends(velocity)
    y_halo = exchange(y_first, y_last, "gy")
    x_halo = exchange(x_first, x_last, "gx")
    z_halo = exchange(z_first, z_last, "gz")
    halos = (x_halo, y_halo, z_halo)
    blocks = {}
    blocks[4], blocks[5] = curl(velocity, (4, 5), pos, 1, 4, halos, with_level=False)
    *rest, level = curl(velocity, (0, 1, 2, 3, 6, 7), pos, 2, 1, halos)
    blocks.update(zip((0, 1, 2, 3, 6, 7), rest))
    side = swap(level, 2)
    across = [(1, 2), (2, 1)]
    outward = [(1, 0), (2, 3)]
    close = chips(level, across)
    distant = chips(level, [(0, 2), (3, 1)])
    close_out = chips(close, outward)
    distant_out = chips(distant, outward)
    mine = [level, side, close + close_out, distant + distant_out]
    theirs = [swap(value, 1) for value in mine]
    got = {0: blocks[0]}
    for m in range(1, 8):
        got[m] = swap(blocks[m], m)
    upper = levels([*mine, *theirs], pos)
    upper = [*upper[:2]] + [jnp.transpose(value, (1, 0, 2)) for value in upper[2:]]
    pencil = None
    for which in LAYS:
        pencil = lay([got[m] for m in which], which, pos, pencil)
    return (jnp.transpose(pencil, (1, 0, 2)), *upper)


LAYS = ((0, 1, 3, 4, 5), (2, 6, 7))


def solution(mesh):
    in_specs = (P(None, "gx", "gy", "gz"),)
    out_specs = (
        P("gx", ("gy", "gz"), None),
        P("gx", "gy", None),
        P("gx", "gy", None),
        P("gx", "gy", None),
        P("gx", "gy", None),
        P("gx", "gy", None),
    )

    return jax.shard_map(
        on_device, mesh=mesh, in_specs=in_specs, out_specs=out_specs, check_vma=False
    )
```

```python
import functools

import jax
import jax.numpy as jnp
from jax import lax
from jax.experimental import pallas as pl
from jax.experimental.pallas import tpu as pltpu
from jax.sharding import PartitionSpec as P


PLANES = 8
HIGHEST = lax.Precision.HIGHEST
F32 = jnp.float32


def pairing(depth):
    row = lax.broadcasted_iota(jnp.int32, (depth, depth // 2), 0)
    col = lax.broadcasted_iota(jnp.int32, (depth, depth // 2), 1)
    return (lax.div(row, jnp.int32(2)) == col).astype(F32)


def pair_lanes(value):
    _, depth = value.shape
    width = min(depth, 256)
    matrix = pairing(width)
    parts = [
        jnp.dot(value[:, i : i + width], matrix, precision=HIGHEST, preferred_element_type=F32)
        for i in range(0, depth, width)
    ]
    return parts[0] if len(parts) == 1 else jnp.concatenate(parts, axis=1)


def keep_rows(scratch, at, value):
    for t in range(scratch.shape[0]):
        scratch[t, at : at + value.shape[0], :] = value[:, t * 128 : (t + 1) * 128]


def pair_rows(scratch, pairs):
    parts = [
        scratch[t, pl.ds(0, pairs, stride=2), :] + scratch[t, pl.ds(1, pairs, stride=2), :]
        for t in range(scratch.shape[0])
    ]
    return parts[0] if len(parts) == 1 else jnp.concatenate(parts, axis=1)


def lanes_at(k, x):
    last = 2 * (k * 32 + x)
    return last, lax.rem(last + 127, 128)


def ends_kernel(
    velocity, x_first, x_last, y_first, y_last, z_first, z_last, uv, w_planes, w_rows, sems
):
    _, X, rows, depth = velocity.shape
    chunk = 4
    chunks = X // chunk
    pieces = [
        (velocity.at[0:2, c * chunk : (c + 1) * chunk], uv.at[:, c * chunk : (c + 1) * chunk])
        for c in range(chunks)
    ]
    pieces += [(velocity.at[2, at], w_planes.at[i]) for i, at in enumerate((0, X - 1))]
    pieces += [
        (velocity.at[2, :, at : at + 8, :], w_rows.at[i]) for i, at in enumerate((0, rows - 8))
    ]
    copies = [pltpu.make_async_copy(a, b, sems.at[i]) for i, (a, b) in enumerate(pieces)]
    for copy in copies:
        copy.start()
    lane = lax.broadcasted_iota(jnp.int32, (rows, 128), 1)
    first = jnp.zeros((rows, 128), F32)
    last = jnp.zeros((rows, 128), F32)
    for c in range(chunks):
        copies[c].wait()
        for p in range(c * chunk, (c + 1) * chunk):
            for k in range(2):
                to_last = 2 * (k * 32 + p)
                to_first = (to_last + 127) % 128
                first = jnp.where(
                    lane == to_first, pltpu.roll(uv[k, p, :, :128], to_first, 1), first
                )
                last = jnp.where(
                    lane == to_last,
                    pltpu.roll(uv[k, p, :, depth - 128 :], (to_last + 1) % 128, 1),
                    last,
                )
            y_first[0, p : p + 1, :] = uv[0, p, 0:1, :]
            y_last[0, p : p + 1, :] = uv[0, p, rows - 1 : rows, :]
    z_first[...] = first
    z_last[...] = last
    for copy in copies[chunks:]:
        copy.wait()
    for i, (out, at) in enumerate(((x_first, 0), (x_last, X - 1))):
        out[0] = uv[1, at]
        out[1] = w_planes[i]
    for p in range(X):
        y_first[1, p : p + 1, :] = w_rows[0, p, 0:1, :]
        y_last[1, p : p + 1, :] = w_rows[1, p, 7:8, :]


def ends(velocity):
    _, X, Y, Z = velocity.shape
    outs = [jax.ShapeDtypeStruct(s, F32) for s in ((2, Y, Z), (2, X, Z), (Y, 128)) for _ in range(2)]
    return pl.pallas_call(
        ends_kernel,
        in_specs=[pl.BlockSpec(memory_space=pl.ANY)],
        out_specs=[pl.BlockSpec(memory_space=pltpu.VMEM)] * 6,
        out_shape=outs,
        scratch_shapes=[
            pltpu.VMEM((2, X, Y, Z), F32),
            pltpu.VMEM((2, Y, Z), F32),
            pltpu.VMEM((2, X, 8, Z), F32),
            pltpu.SemaphoreType.DMA((X // 4 + 4,)),
        ],
        compiler_params=pltpu.CompilerParams(vmem_limit_bytes=53 << 20),
        cost_estimate=pl.CostEstimate(flops=4_000_000, bytes_accessed=8_000_000, transcendentals=0),
        name="ends",
    )(velocity)


def curl_kernel(
    shifts, patched, each, which, pos, vel, v_before, v_after, w_before, w_after, *refs
):
    count = len(shifts)
    if patched:
        x_before, x_after, y_before, y_after, z_before, z_after = refs[:6]
        level_out, turned, summed = refs[-3:]
        outs = refs[6:-3]
        mags, strips = outs[:count], outs[count:]
    else:
        above, below = refs[:2]
        turned = refs[-1]
        mags = refs[2:-1]
    band_at, me = pos[which], pos[0]
    step = pl.program_id(0)
    _, planes, rows, depth = vel.shape
    tall = 2 * each
    tiles = depth // 128
    lane = lax.broadcasted_iota(jnp.int32, (tall, 128), 1)
    at_first, at_last, even_lane = lane == 0, lane == 127, lane % 2 == 0
    at_start = step == 0
    row0 = pl.multiple_of(band_at * rows, 8)
    at_end = step == pl.num_programs(0) - 1

    for pair in range(planes // 2):
        for q in range(rows // tall):
            lo, hi = q * tall, (q + 1) * tall
            band = slice(lo, hi)
            both = []
            here = pl.ds(row0 + lo, tall)
            if patched:
                fills = jnp.where(even_lane, z_before[here, :], z_after[here, :])
            for p in (2 * pair, 2 * pair + 1):

                def first_diff(k):
                    if p + 1 < planes:
                        ahead = vel[k, p + 1, band, :]
                    else:
                        near = (v_after, w_after)[k - 1][0, 0, band, :]
                        ahead = near
                        if patched:
                            ahead = jnp.where(at_end, x_after[k - 1, here, :], near)
                    if p > 0:
                        behind = vel[k, p - 1, band, :]
                    else:
                        near = (v_before, w_before)[k - 1][0, 0, band, :]
                        behind = near
                        if patched:
                            behind = jnp.where(at_start, x_before[k - 1, here, :], near)
                    return ahead - behind

                def second_diff(k):
                    slot = 0 if k == 0 else 1
                    if lo == 0:
                        if patched:
                            edge = y_before[slot, pl.ds(step * planes + p, 1), :]
                        else:
                            edge = above[k, p, 7:8, :]
                        behind = jnp.concatenate([edge, vel[k, p, 0 : hi - 1, :]], axis=0)
                    else:
                        behind = vel[k, p, lo - 1 : hi - 1, :]
                    if hi == rows:
                        if patched:
                            edge = y_after[slot, pl.ds(step * planes + p, 1), :]
                        else:
                            edge = below[k, p, 0:1, :]
                        ahead = jnp.concatenate([vel[k, p, lo + 1 : hi, :], edge], axis=0)
                    else:
                        ahead = vel[k, p, lo + 1 : hi + 1, :]
                    return ahead - behind

                def third_diff(k):
                    fill = jnp.zeros((tall, 128), F32)
                    if patched:
                        last, _ = lanes_at(k, step * planes + p)
                        fill = pltpu.roll(fills, lax.rem(128 - last, 128), 1)
                    parts = [vel[k, p, band, t * 128 : (t + 1) * 128] for t in range(tiles)]
                    on = [pltpu.roll(part, 127, 1) for part in parts] + [fill]
                    back = [fill] + [pltpu.roll(part, 1, 1) for part in parts]
                    return jnp.concatenate(
                        [
                            jnp.where(at_last, on[t + 1], on[t])
                            - jnp.where(at_first, back[t], back[t + 1])
                            for t in range(tiles)
                        ],
                        axis=1,
                    )

                one = second_diff(2) - third_diff(1)
                two = third_diff(0) - first_diff(2)
                three = first_diff(1) - second_diff(0)
                square = 1.0 + 0.25 * (one * one + two * two + three * three)
                mag = square * lax.rsqrt(square)
                both.append(mag)
                for t in range(tiles):
                    turned[t, pl.ds(lo * planes + p, tall, stride=planes), :] = mag[
                        :, t * 128 : (t + 1) * 128
                    ]
            if patched:
                keep_rows(summed, pair * rows + lo, both[0] + both[1])
    if patched:
        level = pair_lanes(pair_rows(summed, planes // 2 * rows // 2)) * 0.125
        level_out[...] = level.reshape(planes // 2, rows // 2, depth // 2)
    size = each * planes
    mask = rows // each - 1
    for m, out in zip(shifts, mags):
        at = pl.multiple_of(size * jnp.bitwise_and(jnp.bitwise_xor(me, m), mask), size)
        for t in range(tiles):
            for y in range(each):
                out[y, :, t * 128 : (t + 1) * 128] = turned[t, pl.ds(at + y * planes, planes), :]
    tile_lane = lax.broadcasted_iota(jnp.int32, (planes, 128), 1)
    for i, m in enumerate(patched):
        ends_out, row_out = strips[2 * i : 2 * i + 2]
        to = jnp.bitwise_xor(me, m)
        at = pl.multiple_of(size * jnp.bitwise_and(to, mask), size)
        edge_row = jnp.where(to == 0, 0, each - 1)
        lanes = jnp.zeros((planes, 128), F32)
        for y in range(each):
            here = pl.ds(at + y * planes, planes)
            for t, lane_to in ((0, 2 * y), (1, (2 * y + 127) % 128)):
                moved = pltpu.roll(turned[t, here, :], 2 * y, 1) if y else turned[t, here, :]
                lanes = jnp.where(tile_lane == lane_to, moved, lanes)
        for k in range(4):

            @pl.when(step == k)
            def _():
                row, col = 24 + k // 2 * 8, k % 2 * 128
                ends_out[row : row + 8, col : col + 128] = lanes

        for t in range(tiles):
            cols = slice(t * 128, (t + 1) * 128)
            row_out[:, cols] = turned[t, pl.ds(at + edge_row * planes, planes), :]
            first = turned[t, pl.ds(at, each, stride=planes), :]
            final = turned[t, pl.ds(at + planes - 1, each, stride=planes), :]

            @pl.when(at_start)
            def _():
                ends_out[0:each, cols] = first

            @pl.when(at_end)
            def _():
                ends_out[each : 2 * each, cols] = final


def curl(velocity, shifts, pos, which, bands, halos=(), patched=(), n=8):
    _, X, Y, Z = velocity.shape
    H = Y // bands
    each = Y // n
    planes = PLANES
    tiles = Z // 128
    halos = [value for pair in halos for value in pair]

    def single(comp, shift):
        def index(i, pos):
            at = jnp.minimum(jnp.maximum(i * planes + shift, 0), X - 1)
            return (comp, at, pos[which], 0)

        return pl.BlockSpec((1, 1, H, Z), index)

    def beside(shift):
        def index(i, pos):
            at = pos[which] * (H // 8) + shift
            return (0, i, jnp.minimum(jnp.maximum(at, 0), Y // 8 - 1), 0)

        return pl.BlockSpec((3, planes, 8, Z), index)

    in_specs = [
        pl.BlockSpec((3, planes, H, Z), lambda i, pos: (0, i, pos[which], 0)),
        single(1, -1),
        single(1, planes),
        single(2, -1),
        single(2, planes),
        *([] if patched else [beside(-1), beside(H // 8)]),
        *[pl.BlockSpec(memory_space=pltpu.VMEM)] * len(halos),
    ]
    args = [velocity] * (5 if patched else 7) + halos
    out_specs = [pl.BlockSpec((each, planes, Z), lambda i, pos: (0, i, 0))] * len(shifts)
    out_shape = [jax.ShapeDtypeStruct((each, X, Z), F32)] * len(shifts)
    scratch = [pltpu.VMEM((tiles, planes * H, 128), F32)]
    for _ in patched:
        out_specs.append(pl.BlockSpec((40, Z), lambda i, pos: (0, 0)))
        out_specs.append(pl.BlockSpec((planes, Z), lambda i, pos: (i, 0)))
        out_shape.append(jax.ShapeDtypeStruct((40, Z), F32))
        out_shape.append(jax.ShapeDtypeStruct((X, Z), F32))
    if patched:
        out_specs.append(pl.BlockSpec((planes // 2, H // 2, Z // 2), lambda i, pos: (i, pos[which], 0)))
        out_shape.append(jax.ShapeDtypeStruct((X // 2, Y // 2, Z // 2), F32))
        scratch.append(pltpu.VMEM((tiles, planes // 2 * H, 128), F32))
    cells = X * H * Z
    return pl.pallas_call(
        functools.partial(curl_kernel, shifts, patched, each, which),
        grid_spec=pltpu.PrefetchScalarGridSpec(
            num_scalar_prefetch=1,
            grid=(X // planes,),
            in_specs=in_specs,
            out_specs=out_specs,
            scratch_shapes=scratch,
        ),
        out_shape=out_shape,
        compiler_params=pltpu.CompilerParams(vmem_limit_bytes=50 << 20),
        cost_estimate=pl.CostEstimate(
            flops=20 * cells, bytes_accessed=20 * cells, transcendentals=cells
        ),
        name="curl",
    )(pos, *args)


def lay_kernel(shifts, pos, *refs):
    blocks = refs[: len(shifts)]
    out, away = refs[-2:]
    depth = blocks[0].shape[2]
    copies = []
    for k, (m, block) in enumerate(zip(shifts, blocks)):
        at = pl.multiple_of(jnp.bitwise_xor(pos[0], m) * depth, depth)
        copies.append(pltpu.make_async_copy(block, out.at[:, :, pl.ds(at, depth)], away.at[k]))
    for copy in copies:
        copy.start()
    for copy in copies:
        copy.wait()


def lay(blocks, shifts, pos, pencil=None, n=8):
    each, X, Z = blocks[0].shape
    count = len(shifts)
    anywhere = pl.BlockSpec(memory_space=pl.ANY)
    in_specs = [pl.BlockSpec(memory_space=pltpu.SMEM)] + [anywhere] * count
    args = [pos, *blocks]
    aliases = {}
    if pencil is not None:
        in_specs.append(anywhere)
        args.append(pencil)
        aliases = {count + 1: 0}
    return pl.pallas_call(
        functools.partial(lay_kernel, shifts),
        in_specs=in_specs,
        out_specs=anywhere,
        out_shape=jax.ShapeDtypeStruct((each, X, n * Z), F32),
        scratch_shapes=[pltpu.SemaphoreType.DMA((count,))],
        compiler_params=pltpu.CompilerParams(vmem_limit_bytes=1 << 20),
        input_output_aliases=aliases,
        cost_estimate=pl.CostEstimate(
            flops=count * each * X * Z, bytes_accessed=8 * count * each * X * Z, transcendentals=0
        ),
        name="lay",
    )(*args)


def patch_kernel(shifts, pos, *refs):
    count = len(shifts)
    blocks, strips = refs[:count], refs[count : 3 * count]
    out, placed, away = refs[-3:]
    each, X, depth = blocks[0].shape
    me = pos[0]
    lane = lax.broadcasted_iota(jnp.int32, (8, 128), 1)
    row = lax.broadcasted_iota(jnp.int32, (8, 128), 0)
    copies = []
    for i, m in enumerate(shifts):
        ends_in, row_in = strips[2 * i : 2 * i + 2]
        for b in range(X // 8):
            lanes = ends_in[24 + b // 2 * 8 : 32 + b // 2 * 8, b % 2 * 128 : (b % 2 + 1) * 128]
            for y in range(each):
                moved = pltpu.roll(lanes, 128 - 2 * y, 1) if y else lanes
                for t in range(2):
                    cols = slice(t * 128, (t + 1) * 128)
                    tile = blocks[i][y, 8 * b : 8 * b + 8, cols]
                    tile = jnp.where(lane == 127 * t, moved, tile)
                    if b == 0:
                        tile = jnp.where(row == 0, ends_in[y : y + 1, cols], tile)
                    if b == X // 8 - 1:
                        tile = jnp.where(row == 7, ends_in[each + y : each + y + 1, cols], tile)
                    if y == 0:
                        tile = jnp.where(me == 0, row_in[8 * b : 8 * b + 8, cols], tile)
                    if y == each - 1:
                        tile = jnp.where(me == 7, row_in[8 * b : 8 * b + 8, cols], tile)
                    placed[i, y, 8 * b : 8 * b + 8, cols] = tile
        at = pl.multiple_of(jnp.bitwise_xor(me, m) * depth, depth)
        copy = pltpu.make_async_copy(placed.at[i], out.at[:, :, pl.ds(at, depth)], away.at[i])
        copy.start()
        copies.append(copy)
    for copy in copies:
        copy.wait()


def patch(blocks, strips, shifts, pos, pencil, n=8):
    each, X, Z = blocks[0].shape
    count = len(shifts)
    vmem, anywhere = pl.BlockSpec(memory_space=pltpu.VMEM), pl.BlockSpec(memory_space=pl.ANY)
    return pl.pallas_call(
        functools.partial(patch_kernel, shifts),
        in_specs=[pl.BlockSpec(memory_space=pltpu.SMEM)] + [vmem] * (3 * count) + [anywhere],
        out_specs=anywhere,
        out_shape=jax.ShapeDtypeStruct((each, X, n * Z), F32),
        scratch_shapes=[pltpu.VMEM((count, each, X, Z), F32), pltpu.SemaphoreType.DMA((count,))],
        input_output_aliases={3 * count + 1: 0},
        compiler_params=pltpu.CompilerParams(vmem_limit_bytes=8 << 20),
        cost_estimate=pl.CostEstimate(
            flops=8 * count * each * X * Z, bytes_accessed=8 * count * each * X * Z, transcendentals=0
        ),
        name="patch",
    )(pos, *blocks, *strips, pencil)


def levels_kernel(pos, *refs):
    blocks = refs[:8]
    one, two, three, four, five, s1, s2, s3, s4 = refs[8:]
    width = blocks[0].shape[2]
    me = pos[0]
    near = jnp.where(me < 4, 4, 2) + jnp.bitwise_and(me, 1)
    far = jnp.where(me < 4, 6, 0) + jnp.bitwise_and(me, 1)
    sources = (me, jnp.bitwise_xor(me, 2), near, far)
    for k, block in enumerate(blocks):
        source = jnp.bitwise_xor(sources[k % 4], k // 4)
        at = pl.multiple_of(source * width, width)
        one[:, :, pl.ds(at, width)] = block[...]

    def up(planes, scratch):
        half, count = len(planes) // 2, planes[0].shape[0]
        for i in range(half):
            keep_rows(scratch, i * count, planes[2 * i] + planes[2 * i + 1])
        result = pair_lanes(pair_rows(scratch, half * count // 2)) * 0.125
        return [result[i * (count // 2) : (i + 1) * (count // 2), :] for i in range(half)]

    planes = up([one[i] for i in range(one.shape[0])], s1)
    for i, plane in enumerate(planes):
        two[i] = plane
    for target, scratch in ((three, s2), (four, s3), (five, s4)):
        planes = up(planes, scratch)
        for i, plane in enumerate(planes):
            for j in range(plane.shape[0]):
                target[j, i : i + 1, :] = plane[j : j + 1, :]


def levels(blocks, pos, n=8):
    planes, rows, width = blocks[0].shape
    depth = width * n
    shapes = [(planes >> k, rows >> k, depth >> k) for k in range(5)]
    outs = shapes[:2] + [(r, p, d) for p, r, d in shapes[2:]]
    vmem = pl.BlockSpec(memory_space=pltpu.VMEM)
    return pl.pallas_call(
        levels_kernel,
        in_specs=[pl.BlockSpec(memory_space=pltpu.SMEM)] + [vmem] * len(blocks),
        out_specs=[vmem] * 5,
        out_shape=[jax.ShapeDtypeStruct(s, F32) for s in outs],
        scratch_shapes=[pltpu.VMEM((s[2] // 128, s[0] // 2 * s[1], 128), F32) for s in shapes[:4]],
        cost_estimate=pl.CostEstimate(
            flops=4 * planes * rows * depth, bytes_accessed=10 * planes * rows * depth, transcendentals=0
        ),
        compiler_params=pltpu.CompilerParams(vmem_limit_bytes=24 << 20),
        name="levels",
    )(pos, *blocks)


def send(value, pairs):
    return lax.ppermute(value, "gz", pairs)


def swap(value, m):
    return send(value, [(i, i ^ m) for i in range(lax.axis_size("gz"))])


def chips(value, pairs):
    return send(value, [(2 * a + core, 2 * b + core) for a, b in pairs for core in (0, 1)])


def exchange(first, last, axis):
    peers = lax.axis_size(axis)
    up = [(i, (i + 1) % peers) for i in range(peers)]
    down = [(j, i) for i, j in up]
    return lax.ppermute(last, axis, up), lax.ppermute(first, axis, down)


def on_device(velocity):
    at = lax.axis_index("gz").astype(jnp.int32)
    pos = jnp.stack([at, lax.shift_right_logical(at, jnp.int32(1)) ^ 2, jnp.int32(0)])
    blocks = {}
    blocks[4], blocks[5] = curl(velocity, (4, 5), pos, 1, 4)
    x_first, x_last, y_first, y_last, z_first, z_last = ends(velocity)
    y_halo = exchange(y_first, y_last, "gy")
    x_halo = exchange(x_first, x_last, "gx")
    z_halo = exchange(z_first, z_last, "gz")
    halos = (x_halo, y_halo, z_halo)
    *rest, ends_4, row_4, ends_5, row_5, level = curl(
        velocity, (0, 1, 2, 3, 6, 7), pos, 2, 1, halos, (4, 5)
    )
    blocks.update(zip((0, 1, 2, 3, 6, 7), rest))
    side = swap(level, 2)
    across = [(1, 2), (2, 1)]
    outward = [(1, 0), (2, 3)]
    close = chips(level, across)
    distant = chips(level, [(0, 2), (3, 1)])
    close_out = chips(close, outward)
    distant_out = chips(distant, outward)
    mine = [level, side, close + close_out, distant + distant_out]
    theirs = [swap(value, 1) for value in mine]
    got = {0: blocks[0]}
    for m in range(1, 8):
        got[m] = swap(blocks[m], m)
    strips = [
        swap(ends_4, 4),
        send(row_4, [(4, 0), (3, 7)]),
        swap(ends_5, 5),
        send(row_5, [(5, 0), (2, 7)]),
    ]
    upper = levels([*mine, *theirs], pos)
    upper = [*upper[:2]] + [jnp.transpose(value, (1, 0, 2)) for value in upper[2:]]
    pencil = lay([got[m] for m in (0, 1, 3)], (0, 1, 3), pos)
    pencil = patch([got[4], got[5]], strips, (4, 5), pos, pencil)
    pencil = lay([got[m] for m in (2, 6, 7)], (2, 6, 7), pos, pencil)
    return (jnp.transpose(pencil, (1, 0, 2)), *upper)


def solution(mesh):
    in_specs = (P(None, "gx", "gy", "gz"),)
    out_specs = (
        P("gx", ("gy", "gz"), None),
        P("gx", "gy", None),
        P("gx", "gy", None),
        P("gx", "gy", None),
        P("gx", "gy", None),
        P("gx", "gy", None),
    )

    return jax.shard_map(
        on_device, mesh=mesh, in_specs=in_specs, out_specs=out_specs, check_vma=False
    )
```
